32 devices in a mesh: sfc: 8 (over z, core), lev: 4 (over y, x).
Axes of the slice: x: 2, y: 2, z: 4, core: 2. Of those that a mesh axis runs over, the one named last changes fastest.
Arguments:
- tracer_old: float32 [4, 10, 16, 3072], P('lev', None, None, 'sfc'), may hold values from 0.1 to 2
- air_old: float32 [4, 16, 3072], P('lev', None, 'sfc'), may hold values from 0.3 to 20, as said below
- air_new: float32 [4, 16, 3072], P('lev', None, 'sfc'), may hold values from 0.4 to 20, as said below
- dep_coord: float32 [2, 4, 16, 3072], P(None, 'lev', None, 'sfc'), may hold values from -1 to 1
- dep_slot: int32 [4, 16, 3072], P('lev', None, 'sfc'), may hold values from 0 to 639
- fetch_list: int32 [8, 2, 128], P('sfc'), may hold values from 0 to 383, as said below
Outputs:
- tracer_new: float32 [4, 10, 16, 3072], P('lev', None, None, 'sfc')
The draws below stay inside these ranges and needn't reach their ends.
Inputs may be any that keep to these rules, and one draw needn't show every extreme that they name: `fetch_list`: side 0 holds distinct indices in [128, 384); side 1 holds distinct indices in [0, 256). `air_old`: positive. `air_new`: positive.
All inputs are finite; a program needn't handle non-finite values.
Results may differ from the reference program's by a relative error of at most 0.0003.
Values sent between devices are 32-bit elements; how exact they have to be, the bound alone decides.
A program may use at most 64 MiB of HBM per device.

```python
import math
import jax
import jax.numpy as jnp
from jax import lax

NP2 = 16
TRACERS = 10
E_DEV = 384
CAP = 128
BAND = 256
SEGS = 8
ELEMS = 3072
LEVELS = 4


def air_ramp():
    levels = jnp.arange(LEVELS, dtype=jnp.float32)
    elems = jnp.arange(ELEMS, dtype=jnp.float32)
    down = 1.0 + 2.0 * levels / max(LEVELS - 1, 1)
    along = 1.0 + 2.0 * elems / ELEMS
    return down[:, None, None] * along[None, None, :]


def draw_air_old(key, part):
    shape = (LEVELS, NP2, ELEMS)
    common = jax.random.uniform(jax.random.fold_in(key, 5), (), jnp.float32, 0.75, 1.25)
    base = jax.random.uniform(key, shape, jnp.float32, 0.8, 1.2)
    return common * base * air_ramp()


def draw_air_new(key, part):
    shape = (LEVELS, NP2, ELEMS)
    inner = jax.random.fold_in(key, 7)
    base = jax.random.uniform(inner, shape, jnp.float32, 0.72, 1.08)
    return base * air_ramp()


def draw_fetch_list(key, part):
    keys = jax.random.split(jax.random.fold_in(key, 11), SEGS * 2)
    orders = jax.vmap(lambda k: jax.random.permutation(k, BAND))(keys)
    picked = orders[:, :CAP].reshape(SEGS, 2, CAP).astype(jnp.int32)
    offset = jnp.array([E_DEV - BAND, 0], dtype=jnp.int32)
    return picked + offset[None, :, None]


def with_ends(values, key, smallest, high):
    longest = values.shape.index(max(values.shape))
    spots = []
    for shift in (0, 1):
        where = [jax.random.randint(jax.random.fold_in(key, axis), (), 0, length) for axis, length in enumerate(values.shape)]
        where[longest] = (where[longest] + shift) % values.shape[longest]
        spots.append(tuple(where))
    return values.at[spots[0]].set(smallest).at[spots[1]].set(high)


def level_of(own_key, dims, shards, smallest, largest):
    factor_of, own = 1.0, jax.random.fold_in(own_key, 6)
    for axis_at, blocks in shards:
        draws = jnp.exp(jax.random.uniform(jax.random.fold_in(own, axis_at), (blocks,), jnp.float32, smallest / len(shards), largest / len(shards)))
        factor_of = factor_of * jnp.repeat(draws, dims[axis_at] // blocks).reshape([-1 if axis == axis_at else 1 for axis in range(len(dims))])
    return factor_of


def setup_inputs(seed: int = 0) -> dict:
    splits = jax.random.split(jax.random.key(seed), 7)
    tracer_old = jnp.clip(jnp.exp(math.log(2.0) - 2.9957323 * jax.random.uniform(splits[0], (LEVELS, TRACERS, NP2, ELEMS), jnp.float32) ** level_of(splits[0], (LEVELS, TRACERS, NP2, ELEMS), ((0, 4), (3, 8)), -0.2, 0.2)), 0.1, 2.0)
    air_old = draw_air_old(jax.random.fold_in(splits[6], 71), 0)
    air_new = draw_air_new(jax.random.fold_in(splits[6], 71), 0)
    dep_coord = jnp.clip(jax.random.uniform(splits[3], (2, LEVELS, NP2, ELEMS), jnp.float32, -1.0, 1.0) * level_of(splits[3], (2, LEVELS, NP2, ELEMS), ((1, 4), (3, 8)), -0.4, 0.0), -1.0, 1.0)
    dep_slot = with_ends(jax.random.randint(splits[4], (LEVELS, NP2, ELEMS), 0, E_DEV + 2 * CAP), jax.random.fold_in(splits[4], 1), 0, (E_DEV + 2 * CAP) - 1).astype(jnp.int32)
    fetch_list = draw_fetch_list(jax.random.fold_in(splits[6], 71), 0)
    return dict(tracer_old=tracer_old, air_old=air_old, air_new=air_new, dep_coord=dep_coord, dep_slot=dep_slot, fetch_list=fetch_list)


NODES = (-1.0, -0.4472135954999579, 0.4472135954999579, 1.0)


def basis(coord):
    terms = []
    for first in range(4):
        term = jnp.ones_like(coord)
        for other in range(4):
            if other != first:
                term = term * (coord - NODES[other]) / (NODES[first] - NODES[other])
        terms.append(term)
    return jnp.stack(terms)


def weights(coord_a, coord_b):
    along_a = basis(coord_a)
    along_b = basis(coord_b)
    stacked = along_a[:, None] * along_b[None, :]
    return stacked.reshape((16,) + coord_a.shape)


def reference(tracer_old, air_old, air_new, dep_coord, dep_slot, fetch_list):
    segs = fetch_list.shape[0]
    total = tracer_old.shape[3]
    e_dev = total // segs
    seg_ids = jnp.arange(segs, dtype=jnp.int32)
    own = seg_ids[:, None] * e_dev + jnp.arange(e_dev, dtype=jnp.int32)[None, :]
    left = ((seg_ids - 1) % segs)[:, None] * e_dev + fetch_list[:, 0]
    right = ((seg_ids + 1) % segs)[:, None] * e_dev + fetch_list[:, 1]
    table = jnp.concatenate([own, left, right], axis=1).astype(jnp.int32)
    seg_of = (jnp.arange(total, dtype=jnp.int32) // e_dev).astype(jnp.int32)
    source = table[seg_of[None, None, :], dep_slot]

    def level(items):
        field, src, coord_a, coord_b = items

        def point(inner):
            index, along_a, along_b = inner
            blocks = jnp.take(field, index, axis=2)
            wts = weights(along_a, along_b)
            value = jnp.sum(wts[None] * blocks, axis=1)
            return value, jnp.min(blocks, axis=1), jnp.max(blocks, axis=1)

        return lax.map(point, (src, coord_a, coord_b))

    interp, low, high = lax.map(level, (tracer_old, source, dep_coord[0], dep_coord[1]))
    interp = jnp.moveaxis(interp, 1, 2)
    low = jnp.moveaxis(low, 1, 2)
    high = jnp.moveaxis(high, 1, 2)
    clipped = jnp.clip(interp, low, high)
    mass_new = air_new[:, None]
    old_mass = jnp.sum(air_old[:, None] * tracer_old, axis=(0, 2, 3))
    clip_mass = jnp.sum(mass_new * clipped, axis=(0, 2, 3))
    room_up = jnp.sum(mass_new * (high - clipped), axis=(0, 2, 3))
    room_down = jnp.sum(mass_new * (clipped - low), axis=(0, 2, 3))
    shortfall = (old_mass - clip_mass)[None, :, None, None]
    raised = shortfall * (high - clipped) / room_up[None, :, None, None]
    lowered = shortfall * (clipped - low) / room_down[None, :, None, None]
    return clipped + jnp.where(shortfall >= 0, raised, lowered)
```

```python
import functools

import jax
import jax.numpy as jnp
from jax import lax
from jax.experimental import pallas as pl
from jax.experimental.pallas import tpu as pltpu
from jax.sharding import PartitionSpec as P

BAND = 256
LANES = 128
SUB = 8
NODES = (-1.0, -0.4472135954999579, 0.4472135954999579, 1.0)
UNROLL = 4
MESH = pl.DeviceIdType.MESH


def basis(coord):
    terms = []
    for first in range(4):
        term = None
        scale = 1.0
        for other in range(4):
            if other != first:
                factor = coord - NODES[other]
                term = factor if term is None else term * factor
                scale = scale / (NODES[first] - NODES[other])
        terms.append(term * scale)
    return terms


def lookup(values, index):
    return jnp.take_along_axis(values, index, axis=1, mode="promise_in_bounds")


def wide(row):
    return jnp.broadcast_to(row, (SUB, LANES))


def kernel(
    sizes, tr, air_old, air_new, coord, slot, fetch, out,
    natural, stage, table, halo, side, along_a, along_b, mixed_a, mixed_b, places, masses, masses_old, coords, wanted,
    kept, message, heard, load_sem, halo_send, halo_recv, sum_send, sum_recv, ready,
):
    n_sfc, n_lev = sizes
    n_all = n_sfc * n_lev
    points = slot.shape[0]
    tracers, _, e_dev = tr.shape
    groups = e_dev // LANES
    row_groups = tracers * points // SUB
    halves = points // SUB
    flat = tracers * SUB
    mains = points
    rests = row_groups - mains
    band_groups = BAND // LANES
    me_s, me_l = lax.axis_index("sfc"), lax.axis_index("lev")
    me = me_s * n_lev + me_l

    barrier = pltpu.get_barrier_semaphore()
    right = (lax.rem(me_s + 1, n_sfc), me_l)
    left = (lax.rem(me_s + n_sfc - 1, n_sfc), me_l)

    def greet(sem, distance):
        for step in (distance, n_sfc - distance):
            pl.semaphore_signal(
                sem, inc=1, device_id=(lax.rem(me_s + step, n_sfc), me_l), device_id_type=MESH
            )

    def greet_levels(sem):
        for distance in range(1, n_lev):
            pl.semaphore_signal(
                sem, inc=1, device_id=(me_s, lax.rem(me_l + distance, n_lev)), device_id_type=MESH
            )

    greet(barrier, 1)
    greet_levels(barrier)

    def cols(group):
        return pl.ds(group * LANES, LANES)

    loads = []

    def load(source, target):
        copy = pltpu.make_async_copy(source, target, load_sem.at[len(loads)])
        copy.start()
        loads.append(copy)

    for g in range(groups):
        for h in range(halves):
            load(tr.at[:, pl.ds(h * SUB, SUB), cols(g)], natural.at[g, h])
        load(slot.at[:, cols(g)], places.at[g])
        load(coord.at[:, :, cols(g)], coords.at[g])
    for g in range(groups):
        load(air_old.at[:, cols(g)], masses_old.at[g])
        load(air_new.at[:, cols(g)], masses.at[g])
    load(fetch, wanted)

    def picked_rows(group):
        if group < mains:
            return pl.ds(group % SUB, SUB, stride=SUB)
        return pl.ds(SUB * SUB + (group - mains) % 2, SUB, stride=2)

    def half_of(h):
        return list(range(SUB * h, SUB * h + SUB)) + [mains + 2 * h, mains + 2 * h + 1]

    tall = tracers * points

    def split(pair):
        value = jnp.concatenate(pair, axis=0)
        high = value.astype(jnp.bfloat16)
        return high, (value - high.astype(jnp.float32)).astype(jnp.bfloat16)

    def prepare():
        for h in range(halves):
            for g in range(groups):
                block = natural.at[g, h].reshape(flat, LANES)
                rows = half_of(h)
                for r, other in zip(rows[::2], rows[1::2]):
                    pair = [block[picked_rows(r), :], block[picked_rows(other), :]]
                    high, low = split(pair)
                    alone = g % 2 == 0 and g + 1 == groups
                    for part, item in enumerate((high, low)):
                        start = (g // 2 * 2 + (0 if alone else part)) * tall + r * SUB
                        at = pl.ds(start, 2 * SUB)
                        table[at, cols(part if alone else g % 2)] = item
        for g in range(groups):
            for i, term in enumerate(basis(coords[g, 0])):
                along_a[i, g] = term
                for s in (0, 1, 4, 5):
                    mixed_a[i // 2, g, pl.ds(s + 2 * (i % 2), points, stride=SUB), :] = term
            for m, term in enumerate(basis(coords[g, 1])):
                along_b[m, g] = term
                for s in (0, 2, 4, 6):
                    mixed_b[m % 2, g, pl.ds(s + m // 2, points, stride=SUB), :] = term

    def shares(point, n, e):
        terms_b = [wide(along_b[m, e, pl.ds(n, 1), :]) for m in range(4)]
        interp = low = high = rest = low_rest = high_rest = None
        for i in range(4):
            inner = None
            for m in range(4):
                value = point(4 * i + m)
                low = value if low is None else jnp.minimum(low, value)
                high = value if high is None else jnp.maximum(high, value)
                scaled = terms_b[m] * value
                inner = scaled if inner is None else inner + scaled
            inner = inner * wide(along_a[i, e, pl.ds(n, 1), :])
            interp = inner if interp is None else interp + inner
        for h in range(halves):
            inner = None
            for q in range(2):
                value = point(mains + 2 * h + q)
                low_rest = value if low_rest is None else jnp.minimum(low_rest, value)
                high_rest = value if high_rest is None else jnp.maximum(high_rest, value)
                scaled = mixed_b[q, e, pl.ds(n * SUB, SUB), :] * value
                inner = scaled if inner is None else inner + scaled
            inner = inner * mixed_a[h, e, pl.ds(n * SUB, SUB), :]
            rest = inner if rest is None else rest + inner
        for shift in (1, 2):
            rest = rest + pltpu.roll(rest, SUB - shift, 0)
            low_rest = jnp.minimum(low_rest, pltpu.roll(low_rest, SUB - shift, 0))
            high_rest = jnp.maximum(high_rest, pltpu.roll(high_rest, SUB - shift, 0))
        return (interp, low, high), (rest, low_rest, high_rest)

    number = lax.broadcasted_iota(jnp.int32, (LANES, LANES), 0).astype(jnp.float32).astype(jnp.bfloat16)

    def chosen(n, e, number, group):
        columns = []
        for p in range(2):
            row = wide(places[e, pl.ds(n + p, 1), :])
            spot = jnp.where(row >> 7 == group, row & (LANES - 1), -1).astype(jnp.float32)
            spot = jnp.concatenate([spot, spot], axis=0).astype(jnp.bfloat16)
            match = number == jnp.concatenate([spot] * SUB, axis=0)
            columns.append(jnp.where(match, jnp.bfloat16(1), jnp.bfloat16(0)))
        return jnp.concatenate(columns, axis=1)

    def times(values, pick):
        return jnp.dot(values, pick, preferred_element_type=jnp.float32)

    def own_found(n, e, number):
        total = None
        for g in range(0, groups, 2):
            one = chosen(n, e, number, g)
            if g + 1 < groups:
                pick = jnp.concatenate([one, chosen(n, e, number, g + 1)], axis=0)
                both = times(table[pl.ds(g * tall, 2 * tall), :], pick)
                found = both[:tall] + both[tall:]
            else:
                pick = jnp.concatenate([one, one], axis=0)
                found = times(table[pl.ds(g * tall, tall), :], pick)
            total = found if total is None else total + found
        return total

    def side_found(at, k, n, e, number):
        one = chosen(n, e, number, groups + k)
        return times(side[at], jnp.concatenate([one, one], axis=0))

    def gather_pass(finder, first, i, carry):
        sums = list(carry)
        n = 2 * i
        for e in range(groups):
            found = finder(n, e, number)
            for p in range(2):
                def point(r):
                    return found[r * SUB : (r + 1) * SUB, p * LANES : (p + 1) * LANES]

                mass = wide(masses[e, pl.ds(n + p, 1), :])
                for b, (value, least, most) in enumerate(shares(point, n + p, e)):
                    clipped = jnp.minimum(jnp.maximum(value, least), most)
                    for q, kind in enumerate((clipped, most - clipped, clipped - least)):
                        sums[3 * b + q] = sums[3 * b + q] + mass * kind
                        if not first:
                            kind = kind + kept[b, q, n + p, :, cols(e)]
                        kept[b, q, n + p, :, cols(e)] = kind
        return tuple(sums)

    def receive(k, h, at):
        for g in range(band_groups):
            pltpu.make_async_copy(halo.at[k, g, h], halo.at[k, g, h], halo_recv.at[k, g, h]).wait()
        index = wide(wanted[pl.ds(k, 1), :]) - jnp.where(k == 0, e_dev - BAND, 0)
        index_low, index_high = index & (LANES - 1), index >> 7
        blocks = [halo.at[k, g, h].reshape(flat, LANES) for g in range(band_groups)]
        rows = half_of(h)
        for first, second in zip(rows[::2], rows[1::2]):
            pair = []
            for r in (first, second):
                value = lookup(blocks[0][picked_rows(r), :], index_low)
                for g in range(1, band_groups):
                    value = jnp.where(
                        index_high == g, lookup(blocks[g][picked_rows(r), :], index_low), value
                    )
                pair.append(value)
            for part, item in enumerate(split(pair)):
                side[at, pl.ds(first * SUB, 2 * SUB), cols(part)] = item

    for copy in loads:
        copy.wait()
    pl.semaphore_wait(barrier, n_lev + 1)
    sends = []
    for k, (target, start) in enumerate(((right, e_dev - BAND), (left, 0))):
        for h in range(halves):
            for g in range(band_groups):
                send = pltpu.make_async_remote_copy(
                    src_ref=natural.at[start // LANES + g, h],
                    dst_ref=halo.at[k, g, h],
                    send_sem=halo_send.at[k, g, h],
                    recv_sem=halo_recv.at[k, g, h],
                    device_id=target,
                    device_id_type=MESH,
                )
                send.start()
                sends.append(send)
    spans = [d for d in (1 << p for p in range(n_sfc)) if 2 * d < n_sfc]

    def next_round(r):
        if 0 < r <= len(spans):
            pl.semaphore_wait(ready.at[r - 1], 2)
        if r < len(spans):
            greet(ready.at[r], spans[r])
        elif r == len(spans):
            greet_levels(ready.at[r])
        else:
            pl.semaphore_wait(ready.at[r - 1], n_lev - 1)

    next_round(0)

    @pl.when(me_s == 0)
    def _():
        next_round(1)

    prepare()
    zero = jnp.zeros((SUB, LANES), jnp.float32)
    sums = lax.fori_loop(
        0, points // 2, functools.partial(gather_pass, own_found, True), (zero,) * 6, unroll=UNROLL
    )

    @pl.when(me_s != 0)
    def _():
        next_round(1)

    lane = lax.broadcasted_iota(jnp.int32, (SUB, LANES), 1)
    row = lax.broadcasted_iota(jnp.int32, (SUB, LANES), 0)
    old_main = jnp.zeros((SUB, LANES), jnp.float32)
    for j in range(mains):
        for g in range(groups):
            block = natural.at[g, j // SUB].reshape(flat, LANES)
            old_main += block[picked_rows(j), :] * wide(masses_old[g, pl.ds(j, 1), :])
    packed = jnp.where(lane == row, jnp.sum(old_main, axis=1, keepdims=True), 0.0)
    for t in range(SUB, tracers):
        product = sum(
            natural[g, h, t] * masses_old[g, pl.ds(h * SUB, SUB), :]
            for g in range(groups)
            for h in range(halves)
        )
        total = jnp.sum(jnp.sum(product, axis=1, keepdims=True), axis=0, keepdims=True)
        at = 4 * (t - SUB)
        packed = jnp.where((lane == 4 * SUB + row) & (row == at), total, packed)

    far = lax.rem(me_s, 2)
    for at, k in enumerate((1 - far, far)):
        for h in range(halves):
            receive(k, h, at)
        sums = lax.fori_loop(
            0,
            points // 2,
            functools.partial(gather_pass, functools.partial(side_found, at, k), False),
            sums,
            unroll=UNROLL,
        )
        if at == 0:
            for r in range(2, len(spans) + 1):
                next_round(r)

    for b in range(2):
        for q in range(3):
            total = jnp.sum(sums[3 * b + q], axis=1, keepdims=True)
            packed = jnp.where(lane == (4 * b + q + 1) * SUB + row, total, packed)
    packed = jnp.sum(packed, axis=0, keepdims=True)
    message[...] = packed

    next_round(len(spans) + 1)

    def tell(place, carry):
        other = place + jnp.where(place >= me, 1, 0)
        pltpu.make_async_remote_copy(
            src_ref=message,
            dst_ref=heard.at[me - jnp.where(place < me, 1, 0)],
            send_sem=sum_send,
            recv_sem=sum_recv,
            device_id=(lax.div(other, n_lev), lax.rem(other, n_lev)),
            device_id_type=MESH,
        ).start()
        return carry

    lax.fori_loop(0, n_all - 1, tell, 0)
    pltpu.make_async_copy(heard, heard, sum_recv).wait()
    total = packed
    for k in range(n_all - 1) if n_all <= 64 else ():
        total = total + heard[k]
    if n_all > 64:
        total = lax.fori_loop(0, n_all - 1, lambda k, acc: acc + heard[k], total)

    old, clip, up, down = [
        wide(total) if q == 0 else pltpu.roll(wide(total), LANES - q * SUB, 1) for q in range(4)
    ]
    shortfall = old - clip
    raised = jnp.where(shortfall >= 0, shortfall / up, 0.0)
    lowered = jnp.where(shortfall >= 0, 0.0, shortfall / down)
    gains = []
    for b in range(2):
        pair = []
        for gain in (raised, lowered):
            column = jnp.where(lane == 4 * b * SUB + row, gain, 0.0)
            pair.append(jnp.broadcast_to(jnp.sum(column, axis=1, keepdims=True), (SUB, LANES)))
        gains.append(pair)

    def fix(n, carry):
        for e in range(groups):
            done = []
            for b in range(2):
                clipped, up, down = [kept[b, q, n, :, cols(e)] for q in range(3)]
                done.append(clipped + (gains[b][0] * up + gains[b][1] * down))
            stage[e, pl.ds(n, SUB, stride=points), :] = done[0]
            for t in range(SUB, tracers):
                at = 4 * (t - SUB)
                stage[e, pl.ds(t * points + n, 1), :] = done[1][at : at + 1]
        return carry

    lax.fori_loop(0, points, fix, 0, unroll=2)
    for g in range(groups):
        out[:, cols(g)] = stage[g]
    for send in sends:
        send.wait_send()
    pltpu.make_async_copy(heard, heard, sum_send).wait()


def solution(mesh):
    sizes = (mesh.shape["sfc"], mesh.shape["lev"])
    n_all = sizes[0] * sizes[1]

    def on_device(tracer_old, air_old, air_new, dep_coord, dep_slot, fetch_list):
        levels, tracers, points, e_dev = tracer_old.shape
        cap = fetch_list.shape[2]
        assert levels == 1 and cap == LANES and tracers == SUB + 2 and points == 16
        rows = tracers * points
        groups, halves = e_dev // LANES, points // SUB
        vmem = pl.BlockSpec(memory_space=pltpu.VMEM)
        result = pl.pallas_call(
            functools.partial(kernel, sizes),
            out_shape=pltpu.VMEM((rows, e_dev), jnp.float32),
            in_specs=[pl.BlockSpec(memory_space=pl.ANY)] * 6,
            out_specs=vmem,
            scratch_shapes=[
                pltpu.VMEM((groups, halves, tracers, SUB, LANES), jnp.float32),
                pltpu.VMEM((groups, rows, LANES), jnp.float32),
                pltpu.VMEM((groups * rows, 2 * LANES), jnp.bfloat16),
                pltpu.VMEM((2, BAND // LANES, halves, tracers, SUB, LANES), jnp.float32),
                pltpu.VMEM((2, rows, 2 * LANES), jnp.bfloat16),
                pltpu.VMEM((4, groups, points, LANES), jnp.float32),
                pltpu.VMEM((4, groups, points, LANES), jnp.float32),
                pltpu.VMEM((2, groups, points * SUB, LANES), jnp.float32),
                pltpu.VMEM((2, groups, points * SUB, LANES), jnp.float32),
                pltpu.VMEM((groups, points, LANES), jnp.int32),
                pltpu.VMEM((groups, points, LANES), jnp.float32),
                pltpu.VMEM((groups, points, LANES), jnp.float32),
                pltpu.VMEM((groups, 2, points, LANES), jnp.float32),
                pltpu.VMEM((2, cap), jnp.int32),
                pltpu.VMEM((2, 3, points, SUB, e_dev), jnp.float32),
                pltpu.VMEM((1, LANES), jnp.float32),
                pltpu.VMEM((n_all - 1, 1, LANES), jnp.float32),
                pltpu.SemaphoreType.DMA(((4 + halves) * groups + 1,)),
                pltpu.SemaphoreType.DMA((2, BAND // LANES, halves)),
                pltpu.SemaphoreType.DMA((2, BAND // LANES, halves)),
                pltpu.SemaphoreType.DMA,
                pltpu.SemaphoreType.DMA,
                pltpu.SemaphoreType.REGULAR((sizes[0].bit_length(),)),
            ],
            compiler_params=pltpu.CompilerParams(collective_id=0, has_side_effects=True),
            name="transport",
        )(
            tracer_old.reshape(tracers, points, e_dev),
            air_old.reshape(points, e_dev),
            air_new.reshape(points, e_dev),
            dep_coord.reshape(2, points, e_dev),
            dep_slot.reshape(points, e_dev),
            fetch_list.reshape(2, cap),
        )
        return result.reshape(levels, tracers, points, e_dev)

    return jax.shard_map(
        on_device,
        mesh=mesh,
        in_specs=(
            P("lev", None, None, "sfc"),
            P("lev", None, "sfc"),
            P("lev", None, "sfc"),
            P(None, "lev", None, "sfc"),
            P("lev", None, "sfc"),
            P("sfc", None, None),
        ),
        out_specs=P("lev", None, None, "sfc"),
        check_vma=False,
    )
```

```python
import functools
import math

import jax
import jax.numpy as jnp
from jax import lax
from jax.experimental import pallas as pl
from jax.experimental.pallas import tpu as pltpu
from jax.sharding import PartitionSpec as P

BAND = 256
LANES = 128
SUB = 8
NODES = (-1.0, -0.4472135954999579, 0.4472135954999579, 1.0)
UNROLL = 8
MESH = pl.DeviceIdType.MESH


def basis(coord):
    terms = []
    for first in range(4):
        term = None
        scale = 1.0
        for other in range(4):
            if other != first:
                factor = coord - NODES[other]
                term = factor if term is None else term * factor
                scale = scale / (NODES[first] - NODES[other])
        terms.append(term * scale)
    return terms


def cubic(values):
    outer, inner = values[3] + values[0], values[2] + values[1]
    wide_odd, near_odd = values[3] - values[0], (values[2] - values[1]) * math.sqrt(5.0)
    return [
        0.625 * inner - 0.125 * outer,
        0.625 * near_odd - 0.125 * wide_odd,
        0.625 * (outer - inner),
        0.625 * (wide_odd - near_odd),
    ]


def horner(terms, at):
    total = terms[3]
    for term in terms[2::-1]:
        total = total * at + term
    return total


def lookup(values, index):
    return jnp.take_along_axis(values, index, axis=1, mode="promise_in_bounds")


def wide(row):
    return jnp.broadcast_to(row, (SUB, LANES))


def split(pair):
    value = jnp.concatenate(pair, axis=0)
    high = value.astype(jnp.bfloat16)
    return high, (value - high.astype(jnp.float32)).astype(jnp.bfloat16)


def folded(values, combine):
    for shift in (1, 2):
        values = combine(values, pltpu.roll(values, SUB - shift, 0))
    return values


def kernel(
    sizes, tr, air_old, air_new, coord, slot, fetch, out,
    natural, stage, table, spare, halo, side, plain, picks, along, places, masses, masses_old, coords, wanted,
    kept, gains, message, heard, load_sem, halo_send, halo_recv, sum_send, sum_recv, ready,
):
    n_sfc, n_lev = sizes
    n_all = n_sfc * n_lev
    points = slot.shape[0]
    tracers, _, e_dev = tr.shape
    groups = e_dev // LANES
    halves = points // SUB
    mains = points
    line = 4
    flat = tracers * points
    kinds = mains + line + 4
    tall = kinds * SUB
    band_groups = BAND // LANES
    steps = points // 2
    me_s, me_l = lax.axis_index("sfc"), lax.axis_index("lev")
    me = me_s * n_lev + me_l
    right = (lax.rem(me_s + 1, n_sfc), me_l)
    left = (lax.rem(me_s + n_sfc - 1, n_sfc), me_l)
    hub_s, hub_l = n_sfc - 1, n_lev - 1
    at_hub = me == n_all - 1
    barrier = pltpu.get_barrier_semaphore()

    def signal(sem, s, l):
        pl.semaphore_signal(sem, inc=1, device_id=(s, l), device_id_type=MESH)

    for other_s, other_l in (right, left):

        @pl.when(jnp.logical_or(other_s != hub_s, other_l != hub_l))
        def _():
            signal(barrier, other_s, other_l)

    @pl.when(jnp.logical_not(at_hub))
    def _():
        signal(barrier, hub_s, hub_l)

    def cols(group):
        return pl.ds(group * LANES, LANES)

    loads = []

    def load(source, target):
        copy = pltpu.make_async_copy(source, target, load_sem.at[len(loads)])
        copy.start()
        loads.append(copy)

    for g in range(groups):
        load(tr.at[:, :, cols(g)], natural.at[g])
    for g in range(groups):
        load(slot.at[:, cols(g)], places.at[g])
        load(coord.at[:, :, cols(g)], coords.at[g])
    for g in range(groups):
        load(air_old.at[:, cols(g)], masses_old.at[g])
        load(air_new.at[:, cols(g)], masses.at[g])
    load(fetch, wanted)

    def picked_rows(r):
        if r < mains:
            return pl.ds(r, SUB, stride=points)
        return pl.ds(SUB * points + (r - mains), SUB, stride=line)

    def as_rows(main, rest):
        ranges = []
        for combine in (jnp.minimum, jnp.maximum):
            ranges.append(functools.reduce(combine, main))
        for combine in (jnp.minimum, jnp.maximum):
            ranges.append(folded(functools.reduce(combine, rest), combine))
        along_b = [cubic(main[line * i : line * i + line]) for i in range(line)]
        along_a = [cubic([along_b[i][m] for i in range(line)]) for m in range(line)]
        return [along_a[m][i] for i in range(line) for m in range(line)] + cubic(rest) + ranges

    def prepare():
        for g in range(groups):
            block = natural.at[g].reshape(flat, LANES)
            found = [block[picked_rows(r), :] for r in range(mains + line)]
            rows = as_rows(found[:mains], found[mains:])
            if g == groups - 1:
                for r, item in enumerate(rows):
                    spare[pl.ds(r * SUB, SUB), :] = item
                continue
            for r in range(0, kinds, 2):
                for part, item in enumerate(split(rows[r : r + 2])):
                    at = pl.ds((g // 2 * 2 + part) * tall + r * SUB, 2 * SUB)
                    table[at, cols(g % 2)] = item
        for g in range(groups):
            for i, term in enumerate(basis(coords[g, 0])):
                for s in (i, i + line):
                    along[g, pl.ds(s, points, stride=SUB), :] = term

    def interpolate(point, n, e):
        at_a, at_b = [wide(coords[e, x, pl.ds(n, 1), :]) for x in range(2)]
        inner = [horner([point(line * i + m) for m in range(line)], at_b) for i in range(line)]
        interp = horner(inner, at_a)
        rest = horner([point(mains + m) for m in range(line)], at_b)
        rest = folded(rest * along[e, pl.ds(n * SUB, SUB), :], jnp.add)
        low, high, low_rest, high_rest = [point(mains + line + x) for x in range(4)]
        return (interp, low, high), (rest, low_rest, high_rest)

    number = lax.broadcasted_iota(jnp.int32, (LANES, LANES), 0).astype(jnp.float32).astype(jnp.bfloat16)

    def chosen(n, e, group):
        columns = []
        for p in range(2):
            row = wide(places[e, pl.ds(n + p, 1), :])
            spot = jnp.where(row >> 7 == group, row & (LANES - 1), -1).astype(jnp.float32)
            spot = jnp.concatenate([spot, spot], axis=0).astype(jnp.bfloat16)
            match = number == jnp.concatenate([spot] * SUB, axis=0)
            columns.append(jnp.where(match, jnp.bfloat16(1), jnp.bfloat16(0)))
        return jnp.concatenate(columns, axis=1)

    def times(values, pick):
        return jnp.dot(values, pick, preferred_element_type=jnp.float32)

    def own_found(n, e):
        total = None
        for g in range(0, groups - 1, 2):
            pick = jnp.concatenate([chosen(n, e, g + x) for x in range(2)], axis=0)
            both = times(table[pl.ds(g * tall, 2 * tall), :], pick)
            found = both[:tall] + both[tall:]
            total = found if total is None else total + found
        return total

    def near_found(k, n, e):
        one = chosen(n, e, groups + k)
        return times(side[0], jnp.concatenate([one, one], axis=0))

    def far_found(n, e):
        one = picks[n // 2, e]
        return times(side[1], jnp.concatenate([one, one], axis=0))

    def foresee(k, i, carry):
        for e in range(groups - 1):
            picks[i, e] = chosen(2 * i, e, groups + k)
        return carry

    def gather_pass(finder, values, group, turn, i, carry):
        sums = list(carry)
        n = 2 * i
        for e in range(groups):
            by_lookup = turn > 0 and e == groups - 1
            found = None if by_lookup else finder(n, e)
            for p in range(2):
                index = wide(places[e, pl.ds(n + p, 1), :])
                low_index, mine = index & (LANES - 1), (index >> 7) == group

                def point(r):
                    here = pl.ds(r * SUB, SUB)
                    if found is not None:
                        value = found[r * SUB : (r + 1) * SUB, p * LANES : (p + 1) * LANES]
                        if turn > 0:
                            return value
                        return jnp.where(mine, lookup(values[here, :], low_index), value)
                    return lookup(values[here, :], low_index)

                mass = wide(masses[e, pl.ds(n + p, 1), :])
                for b, (value, least, most) in enumerate(interpolate(point, n + p, e)):
                    clipped = jnp.minimum(jnp.maximum(value, least), most)
                    for q, kind in enumerate((clipped, most - clipped, clipped - least)):
                        if by_lookup:
                            kind = jnp.where(mine, kind, 0.0)
                        sums[3 * b + q] = sums[3 * b + q] + mass * kind
                        kept[turn, b, q, n + p, :, cols(e)] = kind
        return tuple(sums)

    def receive(k, at):
        index = wide(wanted[pl.ds(k, 1), :]) - jnp.where(k == 0, e_dev - BAND, 0)
        index_low, index_high = index & (LANES - 1), index >> 7
        blocks = [halo.at[k, g].reshape(flat, LANES) for g in range(band_groups)]
        found = []

        def select(r):
            value = lookup(blocks[0][picked_rows(r), :], index_low)
            for g in range(1, band_groups):
                value = jnp.where(
                    index_high == g, lookup(blocks[g][picked_rows(r), :], index_low), value
                )
            found.append(value)

        for h in range(halves):
            for g in range(band_groups):
                landed = halo.at[k, g, :, pl.ds(h * SUB, SUB), :]
                pltpu.make_async_copy(landed, landed, halo_recv.at[k, g, h]).wait()
            for r in range(h * SUB, h * SUB + SUB):
                select(r)
        for r in range(mains, mains + line):
            select(r)
        rows = as_rows(found[:mains], found[mains:])
        for r in range(0, kinds, 2):
            for part, item in enumerate(split(rows[r : r + 2])):
                side[at, pl.ds(r * SUB, 2 * SUB), cols(part)] = item
        for r, item in enumerate(rows):
            plain[at, pl.ds(r * SUB, SUB), :] = item

    for copy in loads:
        copy.wait()
    pl.semaphore_wait(barrier, jnp.where(at_hub, n_all - 1, 2))
    sends = []
    for k, (target, start) in enumerate(((right, e_dev - BAND), (left, 0))):
        for h in range(halves):
            for g in range(band_groups):
                part = pl.ds(h * SUB, SUB)
                send = pltpu.make_async_remote_copy(
                    src_ref=natural.at[start // LANES + g, :, part, :],
                    dst_ref=halo.at[k, g, :, part, :],
                    send_sem=halo_send.at[k, g, h],
                    recv_sem=halo_recv.at[k, g, h],
                    device_id=target,
                    device_id_type=MESH,
                )
                send.start()
                sends.append(send)

    @pl.when(at_hub)
    def _():
        def admit(other, carry):
            signal(ready, lax.div(other, n_lev), lax.rem(other, n_lev))
            return carry

        lax.fori_loop(0, n_all - 1, admit, 0)

    prepare()
    zero = jnp.zeros((SUB, LANES), jnp.float32)
    sums = lax.fori_loop(
        0, steps, functools.partial(gather_pass, own_found, spare, groups - 1, 0), (zero,) * 6, unroll=UNROLL
    )

    lane = lax.broadcasted_iota(jnp.int32, (SUB, LANES), 1)
    row = lax.broadcasted_iota(jnp.int32, (SUB, LANES), 0)
    old_main = jnp.zeros((SUB, LANES), jnp.float32)
    for g in range(groups):
        block = natural.at[g].reshape(flat, LANES)
        for j in range(mains):
            old_main += block[picked_rows(j), :] * wide(masses_old[g, pl.ds(j, 1), :])
    packed = jnp.where(lane == row, jnp.sum(old_main, axis=1, keepdims=True), 0.0)
    for t in range(SUB, tracers):
        product = sum(natural[g, t] * masses_old[g] for g in range(groups))
        total = jnp.sum(jnp.sum(product, axis=1, keepdims=True), axis=0, keepdims=True)
        at = line * (t - SUB)
        packed = jnp.where((lane == 4 * SUB + row) & (row == at), total, packed)

    far = lax.rem(me_s, 2)
    near = 1 - far
    receive(near, 0)
    sums = lax.fori_loop(
        0,
        steps,
        functools.partial(gather_pass, functools.partial(near_found, near), plain.at[0], groups + near, 1),
        sums,
        unroll=UNROLL,
    )
    lax.fori_loop(0, steps, functools.partial(foresee, far), 0, unroll=2)
    receive(far, 1)
    sums = lax.fori_loop(
        0,
        steps,
        functools.partial(gather_pass, far_found, plain.at[1], groups + far, 2),
        sums,
        unroll=UNROLL,
    )

    for b in range(2):
        for q in range(3):
            total = jnp.sum(sums[3 * b + q], axis=1, keepdims=True)
            packed = jnp.where(lane == (4 * b + q + 1) * SUB + row, total, packed)
    packed = jnp.sum(packed, axis=0, keepdims=True)
    message[...] = packed

    @pl.when(jnp.logical_not(at_hub))
    def _():
        pl.semaphore_wait(ready, 1)

    def tell(place, carry):
        other = place + jnp.where(place >= me, 1, 0)
        pltpu.make_async_remote_copy(
            src_ref=message,
            dst_ref=heard.at[me - jnp.where(place < me, 1, 0)],
            send_sem=sum_send,
            recv_sem=sum_recv,
            device_id=(lax.div(other, n_lev), lax.rem(other, n_lev)),
            device_id_type=MESH,
        ).start()
        return carry

    lax.fori_loop(0, n_all - 1, tell, 0)

    def arrange(n, carry):
        for e in range(groups):
            for q in range(3):
                main, rest = [
                    sum(kept[turn, b, q, n, :, cols(e)] for turn in range(3)) for b in range(2)
                ]
                stage[q, e, pl.ds(n, SUB, stride=points), :] = main
                for t in range(SUB, tracers):
                    at = line * (t - SUB)
                    stage[q, e, pl.ds(t * points + n, 1), :] = rest[at : at + 1]
        return carry

    lax.fori_loop(0, points, arrange, 0, unroll=2)
    for send in sends:
        send.wait_send()
    pltpu.make_async_copy(heard, heard, sum_recv).wait()
    total = packed
    for k in range(n_all - 1) if n_all <= 64 else ():
        total = total + heard[k]
    if n_all > 64:
        total = lax.fori_loop(0, n_all - 1, lambda k, acc: acc + heard[k], total)

    old, clip, up, down = [
        wide(total) if q == 0 else pltpu.roll(wide(total), LANES - q * SUB, 1) for q in range(4)
    ]
    shortfall = old - clip
    raised = jnp.where(shortfall >= 0, shortfall / up, 0.0)
    lowered = jnp.where(shortfall >= 0, 0.0, shortfall / down)
    for b in range(2):
        for x, gain in enumerate((raised, lowered)):
            column = jnp.where(lane == 4 * b * SUB + row, gain, 0.0)
            gains[b, x] = jnp.broadcast_to(jnp.sum(column, axis=1, keepdims=True), (SUB, LANES))
    for t in range(tracers):
        b, at = (0, t) if t < SUB else (1, line * (t - SUB))
        up, down = [wide(gains[b, x, pl.ds(at, 1), :]) for x in range(2)]
        for g in range(groups):
            for h in range(halves):
                rows = pl.ds(t * points + h * SUB, SUB)
                moved = up * stage[1, g, rows, :] + down * stage[2, g, rows, :]
                out[rows, cols(g)] = stage[0, g, rows, :] + moved
    pltpu.make_async_copy(heard, heard, sum_send).wait()


def solution(mesh):
    sizes = (mesh.shape["sfc"], mesh.shape["lev"])
    n_all = sizes[0] * sizes[1]

    def on_device(tracer_old, air_old, air_new, dep_coord, dep_slot, fetch_list):
        levels, tracers, points, e_dev = tracer_old.shape
        cap = fetch_list.shape[2]
        assert levels == 1 and cap == LANES and tracers == SUB + 2 and points == 16
        assert e_dev // LANES % 2 == 1
        rows = tracers * points
        groups, halves = e_dev // LANES, points // SUB
        tall = (points + 8) * SUB
        vmem = pl.BlockSpec(memory_space=pltpu.VMEM)
        result = pl.pallas_call(
            functools.partial(kernel, sizes),
            out_shape=pltpu.VMEM((rows, e_dev), jnp.float32),
            in_specs=[pl.BlockSpec(memory_space=pl.ANY)] * 6,
            out_specs=vmem,
            scratch_shapes=[
                pltpu.VMEM((groups, tracers, points, LANES), jnp.float32),
                pltpu.VMEM((3, groups, rows, LANES), jnp.float32),
                pltpu.VMEM(((groups - 1) * tall, 2 * LANES), jnp.bfloat16),
                pltpu.VMEM((tall, LANES), jnp.float32),
                pltpu.VMEM((2, BAND // LANES, tracers, points, LANES), jnp.float32),
                pltpu.VMEM((2, tall, 2 * LANES), jnp.bfloat16),
                pltpu.VMEM((2, tall, LANES), jnp.float32),
                pltpu.VMEM((points // 2, groups - 1, LANES, 2 * LANES), jnp.bfloat16),
                pltpu.VMEM((groups, points * SUB, LANES), jnp.float32),
                pltpu.VMEM((groups, points, LANES), jnp.int32),
                pltpu.VMEM((groups, points, LANES), jnp.float32),
                pltpu.VMEM((groups, points, LANES), jnp.float32),
                pltpu.VMEM((groups, 2, points, LANES), jnp.float32),
                pltpu.VMEM((2, cap), jnp.int32),
                pltpu.VMEM((3, 2, 3, points, SUB, e_dev), jnp.float32),
                pltpu.VMEM((2, 2, SUB, LANES), jnp.float32),
                pltpu.VMEM((1, LANES), jnp.float32),
                pltpu.VMEM((n_all - 1, 1, LANES), jnp.float32),
                pltpu.SemaphoreType.DMA((5 * groups + 1,)),
                pltpu.SemaphoreType.DMA((2, BAND // LANES, halves)),
                pltpu.SemaphoreType.DMA((2, BAND // LANES, halves)),
                pltpu.SemaphoreType.DMA,
                pltpu.SemaphoreType.DMA,
                pltpu.SemaphoreType.REGULAR,
            ],
            compiler_params=pltpu.CompilerParams(collective_id=0, has_side_effects=True),
            name="transport",
        )(
            tracer_old.reshape(tracers, points, e_dev),
            air_old.reshape(points, e_dev),
            air_new.reshape(points, e_dev),
            dep_coord.reshape(2, points, e_dev),
            dep_slot.reshape(points, e_dev),
            fetch_list.reshape(2, cap),
        )
        return result.reshape(levels, tracers, points, e_dev)

    return jax.shard_map(
        on_device,
        mesh=mesh,
        in_specs=(
            P("lev", None, None, "sfc"),
            P("lev", None, "sfc"),
            P("lev", None, "sfc"),
            P(None, "lev", None, "sfc"),
            P("lev", None, "sfc"),
            P("sfc", None, None),
        ),
        out_specs=P("lev", None, None, "sfc"),
        check_vma=False,
    )
```

```python
import functools
import math

import jax
import jax.numpy as jnp
from jax import lax
from jax.experimental import pallas as pl
from jax.experimental.pallas import tpu as pltpu
from jax.sharding import PartitionSpec as P

BAND = 256
LANES = 128
SUB = 8
NODES = (-1.0, -0.4472135954999579, 0.4472135954999579, 1.0)
UNROLL = 8
MESH = pl.DeviceIdType.MESH


def basis(coord):
    terms = []
    for first in range(4):
        term = None
        scale = 1.0
        for other in range(4):
            if other != first:
                factor = coord - NODES[other]
                term = factor if term is None else term * factor
                scale = scale / (NODES[first] - NODES[other])
        terms.append(term * scale)
    return terms


def cubic(values):
    outer, inner = values[3] + values[0], values[2] + values[1]
    wide_odd, near_odd = values[3] - values[0], (values[2] - values[1]) * math.sqrt(5.0)
    return [
        0.625 * inner - 0.125 * outer,
        0.625 * near_odd - 0.125 * wide_odd,
        0.625 * (outer - inner),
        0.625 * (wide_odd - near_odd),
    ]


def horner(terms, at):
    total = terms[3]
    for term in terms[2::-1]:
        total = total * at + term
    return total


def lookup(values, index):
    return jnp.take_along_axis(values, index, axis=1, mode="promise_in_bounds")


def wide(row):
    return jnp.broadcast_to(row, (SUB, LANES))


def split(pair):
    value = jnp.concatenate(pair, axis=0)
    high = value.astype(jnp.bfloat16)
    return high, (value - high.astype(jnp.float32)).astype(jnp.bfloat16)


def folded(values, combine):
    for shift in (1, 2):
        values = combine(values, pltpu.roll(values, SUB - shift, 0))
    return values


def kernel(
    sizes, tr, air_old, air_new, coord, slot, fetch, out,
    fields, stage, table, spare, halo, side, plain, picks, along, places, wanted,
    kept, gains, message, heard, load_sem, halo_send, halo_recv, sum_send, sum_recv, ready,
):
    n_sfc, n_lev = sizes
    n_all = n_sfc * n_lev
    points = slot.shape[0]
    tracers, _, e_dev = tr.shape
    groups = e_dev // LANES
    halves = points // SUB
    mains = points
    line = 4
    flat = tracers * points
    kinds = mains + line + 4
    tall = kinds * SUB
    main_tall = (mains + 2) * SUB
    band_groups = BAND // LANES
    steps = points // 2
    me_s, me_l = lax.axis_index("sfc"), lax.axis_index("lev")
    me = me_s * n_lev + me_l
    right = (lax.rem(me_s + 1, n_sfc), me_l)
    left = (lax.rem(me_s + n_sfc - 1, n_sfc), me_l)
    hub_s, hub_l = n_sfc - 1, n_lev - 1
    at_hub = me == n_all - 1
    far = lax.rem(me_s, 2)
    near = 1 - far
    barrier = pltpu.get_barrier_semaphore()

    def signal(sem, s, l):
        pl.semaphore_signal(sem, inc=1, device_id=(s, l), device_id_type=MESH)

    for other_s, other_l in (right, left):

        @pl.when(jnp.logical_or(other_s != hub_s, other_l != hub_l))
        def _():
            signal(barrier, other_s, other_l)

    @pl.when(jnp.logical_not(at_hub))
    def _():
        signal(barrier, hub_s, hub_l)

    def cols(group):
        return pl.ds(group * LANES, LANES)

    def load(source, target, sem):
        pltpu.make_async_copy(source, target, load_sem.at[sem]).start()

    at_coord, at_new, at_old = tracers, tracers + 2, tracers + 3
    for g in range(groups):
        load(tr.at[:, :, cols(g)], fields.at[g, pl.ds(0, tracers)], 0)
    for g in range(groups):
        load(slot.at[:, cols(g)], places.at[g], 1)
        load(coord.at[:, :, cols(g)], fields.at[g, pl.ds(at_coord, 2)], 0)
    for g in range(groups):
        load(air_old.at[:, cols(g)], fields.at[g, at_old], 0)
        load(air_new.at[:, cols(g)], fields.at[g, at_new], 0)
    load(fetch, wanted, 2)

    def picked_rows(r):
        if r < mains:
            return pl.ds(r, SUB, stride=points)
        return pl.ds(SUB * points + (r - mains), SUB, stride=line)

    def main_rows(main):
        along_b = [cubic(main[line * i : line * i + line]) for i in range(line)]
        along_a = [cubic([along_b[i][m] for i in range(line)]) for m in range(line)]
        ranges = [functools.reduce(combine, main) for combine in (jnp.minimum, jnp.maximum)]
        return [along_a[m][i] for i in range(line) for m in range(line)] + ranges

    def rest_rows(rest):
        return cubic(rest) + [
            folded(functools.reduce(combine, rest), combine) for combine in (jnp.minimum, jnp.maximum)
        ]

    def prepare():
        for g in range(groups):
            block = fields.at[g].reshape((tracers + 4) * points, LANES)
            found = [block[picked_rows(r), :] for r in range(mains + line)]
            rows = main_rows(found[:mains]) + rest_rows(found[mains:])
            if g == groups - 1:
                for r, item in enumerate(rows):
                    spare[pl.ds(r * SUB, SUB), :] = item
                continue
            for r in range(0, kinds, 2):
                for part, item in enumerate(split(rows[r : r + 2])):
                    at = pl.ds((g // 2 * 2 + part) * tall + r * SUB, 2 * SUB)
                    table[at, cols(g % 2)] = item
        for g in range(groups):
            for i, term in enumerate(basis(fields[g, at_coord])):
                for s in (i, i + line):
                    along[g, pl.ds(s, points, stride=SUB), :] = term

    def interpolate(point, n, e, b):
        at_a, at_b = [wide(fields[e, at_coord + x, pl.ds(n, 1), :]) for x in range(2)]
        if b == 0:
            inner = [horner([point(line * i + m) for m in range(line)], at_b) for i in range(line)]
            return horner(inner, at_a), point(mains), point(mains + 1)
        rest = horner([point(mains + 2 + m) for m in range(line)], at_b)
        rest = folded(rest * along[e, pl.ds(n * SUB, SUB), :], jnp.add)
        return rest, point(mains + 2 + line), point(mains + 3 + line)

    number = lax.broadcasted_iota(jnp.int32, (LANES, LANES), 0).astype(jnp.float32).astype(jnp.bfloat16)

    def chosen(n, e, group):
        columns = []
        for p in range(2):
            row = wide(places[e, pl.ds(n + p, 1), :])
            spot = jnp.where(row >> 7 == group, row & (LANES - 1), -1).astype(jnp.float32)
            spot = jnp.concatenate([spot, spot], axis=0).astype(jnp.bfloat16)
            match = number == jnp.concatenate([spot] * SUB, axis=0)
            columns.append(jnp.where(match, jnp.bfloat16(1), jnp.bfloat16(0)))
        return jnp.concatenate(columns, axis=1)

    def times(values, pick):
        return jnp.dot(values, pick, preferred_element_type=jnp.float32)

    def own_found(n, e):
        total = None
        for g in range(0, groups - 1, 2):
            pick = jnp.concatenate([chosen(n, e, g + x) for x in range(2)], axis=0)
            both = times(table[pl.ds(g * tall, 2 * tall), :], pick)
            found = both[:tall] + both[tall:]
            total = found if total is None else total + found
        return total

    def near_found(k, n, e):
        one = chosen(n, e, groups + k)
        return times(side[0], jnp.concatenate([one, one], axis=0))

    def far_found(n, e):
        one = picks[n // 2, e]
        return times(side[1, pl.ds(0, main_tall), :], jnp.concatenate([one, one], axis=0))

    def foresee(k, i, carry):
        for e in range(groups - 1):
            picks[i, e] = chosen(2 * i, e, groups + k)
        return carry

    def gather_pass(finder, values, group, turn, parts, i, carry):
        sums = list(carry)
        n = 2 * i
        for e in range(groups):
            by_lookup = finder is None or (turn > 0 and e == groups - 1)
            found = None if by_lookup else finder(n, e)
            for p in range(2):
                index = wide(places[e, pl.ds(n + p, 1), :])
                low_index, mine = index & (LANES - 1), (index >> 7) == group

                def point(r):
                    here = pl.ds(r * SUB, SUB)
                    if found is not None:
                        value = found[r * SUB : (r + 1) * SUB, p * LANES : (p + 1) * LANES]
                        if turn > 0:
                            return value
                        return jnp.where(mine, lookup(values[here, :], low_index), value)
                    return lookup(values[here, :], low_index)

                mass = wide(fields[e, at_new, pl.ds(n + p, 1), :])
                for b in parts:
                    value, least, most = interpolate(point, n + p, e, b)
                    clipped = jnp.minimum(jnp.maximum(value, least), most)
                    for q, kind in enumerate((clipped, most - clipped, clipped - least)):
                        if by_lookup:
                            kind = jnp.where(mine, kind, 0.0)
                        sums[3 * b + q] = sums[3 * b + q] + mass * kind
                        kept[turn, b, q, n + p, :, cols(e)] = kind
        return tuple(sums)

    def pieces():
        yield pl.ds(SUB, tracers - SUB), pl.ds(0, points)
        for h in range(halves):
            yield pl.ds(0, SUB), pl.ds(h * SUB, SUB)

    def arrived(k, piece):
        landed = halo.at[(k, slice(None), *list(pieces())[piece])]
        pltpu.make_async_copy(landed, landed, halo_recv.at[k, piece]).wait()

    def select(k, rows):
        index = wide(wanted[pl.ds(k, 1), :]) - jnp.where(k == 0, e_dev - BAND, 0)
        index_low, index_high = index & (LANES - 1), index >> 7
        blocks = [halo.at[k, g].reshape(flat, LANES) for g in range(band_groups)]
        found = []
        for r in rows:
            value = lookup(blocks[0][picked_rows(r), :], index_low)
            for g in range(1, band_groups):
                value = jnp.where(
                    index_high == g, lookup(blocks[g][picked_rows(r), :], index_low), value
                )
            found.append(value)
        return found

    def keep(at, start, rows, dense):
        for r in range(0, len(rows), 2) if dense else ():
            for part, item in enumerate(split(rows[r : r + 2])):
                side[at, pl.ds((start + r) * SUB, 2 * SUB), cols(part)] = item
        for r, item in enumerate(rows):
            plain[at, pl.ds((start + r) * SUB, SUB), :] = item

    def receive_rest(k, at, dense):
        arrived(k, 0)
        keep(at, mains + 2, rest_rows(select(k, range(mains, mains + line))), dense)

    def receive_main(k, at):
        found = []
        for h in range(halves):
            arrived(k, 1 + h)
            found += select(k, range(h * SUB, h * SUB + SUB))
        keep(at, 0, main_rows(found), True)

    for sem, filled in enumerate((fields, places, wanted)):
        pltpu.make_async_copy(filled, filled, load_sem.at[sem]).wait()
    pl.semaphore_wait(barrier, jnp.where(at_hub, n_all - 1, 2))
    for k in (near, far):
        ahead = k == 0
        target = (jnp.where(ahead, right[0], left[0]), me_l)
        start = jnp.where(ahead, groups - band_groups, 0)
        for piece, where in enumerate(pieces()):
            for g in range(band_groups):
                pltpu.make_async_remote_copy(
                    src_ref=fields.at[(start + g, *where)],
                    dst_ref=halo.at[(k, g, *where)],
                    send_sem=halo_send,
                    recv_sem=halo_recv.at[k, piece],
                    device_id=target,
                    device_id_type=MESH,
                ).start()

    @pl.when(at_hub)
    def _():
        def admit(other, carry):
            signal(ready, lax.div(other, n_lev), lax.rem(other, n_lev))
            return carry

        lax.fori_loop(0, n_all - 1, admit, 0)

    prepare()
    zero = jnp.zeros((SUB, LANES), jnp.float32)
    sums = lax.fori_loop(
        0, steps, functools.partial(gather_pass, own_found, spare, groups - 1, 0, (0, 1)), (zero,) * 6, unroll=UNROLL
    )

    lane = lax.broadcasted_iota(jnp.int32, (SUB, LANES), 1)
    row = lax.broadcasted_iota(jnp.int32, (SUB, LANES), 0)
    old_main = jnp.zeros((SUB, LANES), jnp.float32)
    for g in range(groups):
        block = fields.at[g].reshape((tracers + 4) * points, LANES)
        for j in range(mains):
            old_main += block[picked_rows(j), :] * wide(fields[g, at_old, pl.ds(j, 1), :])
    old_rest = jnp.zeros((SUB, LANES), jnp.float32)
    for t in range(SUB, tracers):
        product = sum(fields[g, t] * fields[g, at_old] for g in range(groups))
        total = jnp.sum(product, axis=0, keepdims=True)
        old_rest = jnp.where(row == line * (t - SUB), wide(total), old_rest)

    receive_rest(near, 0, True)
    receive_main(near, 0)
    sums = lax.fori_loop(
        0,
        steps,
        functools.partial(gather_pass, functools.partial(near_found, near), plain.at[0], groups + near, 1, (0, 1)),
        sums,
        unroll=UNROLL,
    )
    lax.fori_loop(0, steps, functools.partial(foresee, far), 0, unroll=2)
    receive_rest(far, 1, False)
    sums = lax.fori_loop(
        0, steps, functools.partial(gather_pass, None, plain.at[1], groups + far, 2, (1,)), sums, unroll=UNROLL
    )
    receive_main(far, 1)
    sums = lax.fori_loop(
        0,
        steps,
        functools.partial(gather_pass, far_found, plain.at[1], groups + far, 2, (0,)),
        sums,
        unroll=UNROLL,
    )

    half = LANES // 2
    deficit = room = jnp.zeros((SUB, LANES), jnp.float32)
    for b, old in enumerate((old_main, old_rest)):
        gap, up, down = [
            jnp.sum(item, axis=1, keepdims=True) for item in (old - sums[3 * b], sums[3 * b + 1], sums[3 * b + 2])
        ]
        here, there = lane == b * SUB + row, lane == half + b * SUB + row
        deficit = jnp.where(jnp.logical_or(here, there), gap, deficit)
        room = jnp.where(here, up, jnp.where(there, down, room))
    packed = [jnp.sum(item, axis=0, keepdims=True) for item in (deficit, room)]
    for x in range(2):
        message[pl.ds(x, 1), :] = packed[x]

    @pl.when(jnp.logical_not(at_hub))
    def _():
        pl.semaphore_wait(ready, 1)

    def tell(place, carry):
        other = place + jnp.where(place >= me, 1, 0)
        pltpu.make_async_remote_copy(
            src_ref=message,
            dst_ref=heard.at[me - jnp.where(place < me, 1, 0)],
            send_sem=sum_send,
            recv_sem=sum_recv,
            device_id=(lax.div(other, n_lev), lax.rem(other, n_lev)),
            device_id_type=MESH,
        ).start()
        return carry

    lax.fori_loop(0, n_all - 1, tell, 0)

    def arrange(n, carry):
        for e in range(groups):
            for q in range(3):
                main, rest = [
                    sum(kept[turn, b, q, n, :, cols(e)] for turn in range(3)) for b in range(2)
                ]
                stage[q, e, pl.ds(n, SUB, stride=points), :] = main
                for t in range(SUB, tracers):
                    at = line * (t - SUB)
                    stage[q, e, pl.ds(t * points + n, 1), :] = rest[at : at + 1]
        return carry

    lax.fori_loop(0, points, arrange, 0, unroll=2)
    pltpu.make_async_copy(halo, halo, halo_send).wait()
    pltpu.make_async_copy(heard, heard, sum_recv).wait()
    totals = []
    for x in range(2):
        if n_all <= 64:
            terms = [wide(packed[x])] + [wide(heard[k, pl.ds(x, 1), :]) for k in range(n_all - 1)]
            while len(terms) > 1:
                terms = [sum(terms[k : k + 2]) for k in range(0, len(terms), 2)]
            totals.append(terms[0])
        else:
            totals.append(
                lax.fori_loop(
                    0, n_all - 1, lambda k, acc: acc + wide(heard[k, pl.ds(x, 1), :]), wide(packed[x])
                )
            )
    shortfall, room = totals
    raises = (shortfall >= 0) == (lane < half)
    gain = jnp.where(raises, shortfall / room, 0.0)
    for b in range(2):
        for x in range(2):
            column = jnp.where(lane == half * x + b * SUB + row, gain, 0.0)
            gains[b, x] = jnp.broadcast_to(jnp.sum(column, axis=1, keepdims=True), (SUB, LANES))
    for t in range(tracers):
        b, at = (0, t) if t < SUB else (1, line * (t - SUB))
        up, down = [wide(gains[b, x, pl.ds(at, 1), :]) for x in range(2)]
        for g in range(groups):
            for h in range(halves):
                rows = pl.ds(t * points + h * SUB, SUB)
                moved = up * stage[1, g, rows, :] + down * stage[2, g, rows, :]
                out[rows, cols(g)] = stage[0, g, rows, :] + moved
    pltpu.make_async_copy(heard, heard, sum_send).wait()


def solution(mesh):
    sizes = (mesh.shape["sfc"], mesh.shape["lev"])
    n_all = sizes[0] * sizes[1]

    def on_device(tracer_old, air_old, air_new, dep_coord, dep_slot, fetch_list):
        levels, tracers, points, e_dev = tracer_old.shape
        cap = fetch_list.shape[2]
        assert levels == 1 and cap == LANES and tracers == SUB + 2 and points == 16
        assert e_dev // LANES % 2 == 1
        rows = tracers * points
        groups, halves = e_dev // LANES, points // SUB
        tall = (points + 8) * SUB
        vmem = pl.BlockSpec(memory_space=pltpu.VMEM)
        result = pl.pallas_call(
            functools.partial(kernel, sizes),
            out_shape=pltpu.VMEM((rows, e_dev), jnp.float32),
            in_specs=[pl.BlockSpec(memory_space=pl.ANY)] * 6,
            out_specs=vmem,
            scratch_shapes=[
                pltpu.VMEM((groups, tracers + 4, points, LANES), jnp.float32),
                pltpu.VMEM((3, groups, rows, LANES), jnp.float32),
                pltpu.VMEM(((groups - 1) * tall, 2 * LANES), jnp.bfloat16),
                pltpu.VMEM((tall, LANES), jnp.float32),
                pltpu.VMEM((2, BAND // LANES, tracers, points, LANES), jnp.float32),
                pltpu.VMEM((2, tall, 2 * LANES), jnp.bfloat16),
                pltpu.VMEM((2, tall, LANES), jnp.float32),
                pltpu.VMEM((points // 2, groups - 1, LANES, 2 * LANES), jnp.bfloat16),
                pltpu.VMEM((groups, points * SUB, LANES), jnp.float32),
                pltpu.VMEM((groups, points, LANES), jnp.int32),
                pltpu.VMEM((2, cap), jnp.int32),
                pltpu.VMEM((3, 2, 3, points, SUB, e_dev), jnp.float32),
                pltpu.VMEM((2, 2, SUB, LANES), jnp.float32),
                pltpu.VMEM((2, LANES), jnp.float32),
                pltpu.VMEM((n_all - 1, 2, LANES), jnp.float32),
                pltpu.SemaphoreType.DMA((3,)),
                pltpu.SemaphoreType.DMA,
                pltpu.SemaphoreType.DMA((2, 1 + halves)),
                pltpu.SemaphoreType.DMA,
                pltpu.SemaphoreType.DMA,
                pltpu.SemaphoreType.REGULAR,
            ],
            compiler_params=pltpu.CompilerParams(collective_id=0, has_side_effects=True),
            name="transport",
        )(
            tracer_old.reshape(tracers, points, e_dev),
            air_old.reshape(points, e_dev),
            air_new.reshape(points, e_dev),
            dep_coord.reshape(2, points, e_dev),
            dep_slot.reshape(points, e_dev),
            fetch_list.reshape(2, cap),
        )
        return result.reshape(levels, tracers, points, e_dev)

    return jax.shard_map(
        on_device,
        mesh=mesh,
        in_specs=(
            P("lev", None, None, "sfc"),
            P("lev", None, "sfc"),
            P("lev", None, "sfc"),
            P(None, "lev", None, "sfc"),
            P("lev", None, "sfc"),
            P("sfc", None, None),
        ),
        out_specs=P("lev", None, None, "sfc"),
        check_vma=False,
    )
```

```python
import functools
import math

import jax
import jax.numpy as jnp
from jax import lax
from jax.experimental import pallas as pl
from jax.experimental.pallas import tpu as pltpu
from jax.sharding import PartitionSpec as P

BAND = 256
LANES = 128
SUB = 8
NODES = (-1.0, -0.4472135954999579, 0.4472135954999579, 1.0)
UNROLL = 8
MESH = pl.DeviceIdType.MESH


def basis(coord):
    terms = []
    for first in range(4):
        term = None
        scale = 1.0
        for other in range(4):
            if other != first:
                factor = coord - NODES[other]
                term = factor if term is None else term * factor
                scale = scale / (NODES[first] - NODES[other])
        terms.append(term * scale)
    return terms


def cubic(values):
    outer, inner = values[3] + values[0], values[2] + values[1]
    wide_odd, near_odd = values[3] - values[0], (values[2] - values[1]) * math.sqrt(5.0)
    return [
        0.625 * inner - 0.125 * outer,
        0.625 * near_odd - 0.125 * wide_odd,
        0.625 * (outer - inner),
        0.625 * (wide_odd - near_odd),
    ]


def horner(terms, at):
    total = terms[3]
    for term in terms[2::-1]:
        total = total * at + term
    return total


def lookup(values, index):
    return jnp.take_along_axis(values, index, axis=1, mode="promise_in_bounds")


def wide(row):
    return jnp.broadcast_to(row, (SUB, LANES))


def split(pair):
    value = jnp.concatenate(pair, axis=0)
    high = value.astype(jnp.bfloat16)
    return high, (value - high.astype(jnp.float32)).astype(jnp.bfloat16)


def folded(values, combine):
    for shift in (1, 2):
        values = combine(values, pltpu.roll(values, SUB - shift, 0))
    return values


def kernel(
    sizes, tr, air_old, air_new, coord, slot, fetch, out,
    fields, stage, table, spare, halo, side, plain, picks, along, lagrange, begun, places, wanted,
    kept, gains, message, heard, load_sem, halo_send, halo_recv, sum_send, sum_recv, ready,
):
    n_sfc, n_lev = sizes
    n_all = n_sfc * n_lev
    points = slot.shape[0]
    tracers, _, e_dev = tr.shape
    groups = e_dev // LANES
    halves = points // SUB
    mains = points
    line = 4
    flat = tracers * points
    kinds = mains + line + 4
    tall = kinds * SUB
    half_rows = mains // 2
    band_groups = BAND // LANES
    steps = points // 2
    me_s, me_l = lax.axis_index("sfc"), lax.axis_index("lev")
    me = me_s * n_lev + me_l
    right = (lax.rem(me_s + 1, n_sfc), me_l)
    left = (lax.rem(me_s + n_sfc - 1, n_sfc), me_l)
    hub_s, hub_l = n_sfc - 1, n_lev - 1
    at_hub = me == n_all - 1
    far = lax.rem(me_s, 2)
    near = 1 - far
    barrier = pltpu.get_barrier_semaphore()

    def signal(sem, s, l):
        pl.semaphore_signal(sem, inc=1, device_id=(s, l), device_id_type=MESH)

    for other_s, other_l in (right, left):

        @pl.when(jnp.logical_or(other_s != hub_s, other_l != hub_l))
        def _():
            signal(barrier, other_s, other_l)

    @pl.when(jnp.logical_not(at_hub))
    def _():
        signal(barrier, hub_s, hub_l)

    def cols(group):
        return pl.ds(group * LANES, LANES)

    def load(source, target, sem):
        pltpu.make_async_copy(source, target, load_sem.at[sem]).start()

    at_coord, at_new, at_old = tracers, tracers + 2, tracers + 3
    for g in range(groups):
        load(tr.at[:, :, cols(g)], fields.at[g, pl.ds(0, tracers)], 0)
    for g in range(groups):
        load(slot.at[:, cols(g)], places.at[g], 1)
        load(coord.at[:, :, cols(g)], fields.at[g, pl.ds(at_coord, 2)], 0)
    for g in range(groups):
        load(air_old.at[:, cols(g)], fields.at[g, at_old], 0)
        load(air_new.at[:, cols(g)], fields.at[g, at_new], 0)
    load(fetch, wanted, 2)

    def picked_rows(r):
        if r < mains:
            return pl.ds(r, SUB, stride=points)
        return pl.ds(SUB * points + (r - mains), SUB, stride=line)

    def main_rows(main):
        along_b = [cubic(main[line * i : line * i + line]) for i in range(line)]
        along_a = [cubic([along_b[i][m] for i in range(line)]) for m in range(line)]
        ranges = [functools.reduce(combine, main) for combine in (jnp.minimum, jnp.maximum)]
        return [along_a[m][i] for i in range(line) for m in range(line)] + ranges

    def rest_rows(rest):
        return cubic(rest) + [
            folded(functools.reduce(combine, rest), combine) for combine in (jnp.minimum, jnp.maximum)
        ]

    def prepare():
        for g in range(groups):
            block = fields.at[g].reshape((tracers + 4) * points, LANES)
            found = [block[picked_rows(r), :] for r in range(mains + line)]
            rows = main_rows(found[:mains]) + rest_rows(found[mains:])
            if g == groups - 1:
                for r, item in enumerate(rows):
                    spare[pl.ds(r * SUB, SUB), :] = item
                continue
            for r in range(0, kinds, 2):
                for part, item in enumerate(split(rows[r : r + 2])):
                    at = pl.ds((g // 2 * 2 + part) * tall + r * SUB, 2 * SUB)
                    table[at, cols(g % 2)] = item
        for g in range(groups):
            for i, term in enumerate(basis(fields[g, at_coord])):
                lagrange[i, g] = term
                for s in (i, i + line):
                    along[g, pl.ds(s, points, stride=SUB), :] = term

    def interpolate(point, n, e, b):
        at_a, at_b = [wide(fields[e, at_coord + x, pl.ds(n, 1), :]) for x in range(2)]
        if b == 0:
            inner = [horner([point(line * i + m) for m in range(line)], at_b) for i in range(line)]
            return horner(inner, at_a), point(mains), point(mains + 1)
        rest = horner([point(mains + 2 + m) for m in range(line)], at_b)
        rest = folded(rest * along[e, pl.ds(n * SUB, SUB), :], jnp.add)
        return rest, point(mains + 2 + line), point(mains + 3 + line)

    def half_sum(point, n, e, h):
        at_b = wide(fields[e, at_coord + 1, pl.ds(n, 1), :])
        pair = [
            horner([point(line * x + m) for m in range(line)], at_b)
            * wide(lagrange[2 * h + x, e, pl.ds(n, 1), :])
            for x in range(2)
        ]
        return pair[0] + pair[1]

    def end_sum(point, n, e, b):
        value = begun[n, :, cols(e)] + half_sum(point, n, e, 1)
        return value, point(half_rows), point(half_rows + 1)

    number = lax.broadcasted_iota(jnp.int32, (LANES, LANES), 0).astype(jnp.float32).astype(jnp.bfloat16)

    def chosen(n, e, group):
        columns = []
        for p in range(2):
            row = wide(places[e, pl.ds(n + p, 1), :])
            spot = jnp.where(row >> 7 == group, row & (LANES - 1), -1).astype(jnp.float32)
            spot = jnp.concatenate([spot, spot], axis=0).astype(jnp.bfloat16)
            match = number == jnp.concatenate([spot] * SUB, axis=0)
            columns.append(jnp.where(match, jnp.bfloat16(1), jnp.bfloat16(0)))
        return jnp.concatenate(columns, axis=1)

    def times(values, pick):
        return jnp.dot(values, pick, preferred_element_type=jnp.float32)

    def own_found(n, e):
        total = None
        for g in range(0, groups - 1, 2):
            pick = jnp.concatenate([chosen(n, e, g + x) for x in range(2)], axis=0)
            both = times(table[pl.ds(g * tall, 2 * tall), :], pick)
            found = both[:tall] + both[tall:]
            total = found if total is None else total + found
        return total

    def near_found(k, n, e):
        one = chosen(n, e, groups + k)
        return times(side[0], jnp.concatenate([one, one], axis=0))

    def far_found(first, count, n, e):
        one = picks[n // 2, e]
        values = side[1, pl.ds(first * SUB, count * SUB), :]
        return times(values, jnp.concatenate([one, one], axis=0))

    def foresee(k, i, carry):
        for e in range(groups - 1):
            picks[i, e] = chosen(2 * i, e, groups + k)
        return carry

    def gather_pass(finder, values, group, turn, parts, blend, i, carry):
        sums = list(carry)
        n = 2 * i
        for e in range(groups):
            by_lookup = finder is None or (turn > 0 and e == groups - 1)
            found = None if by_lookup else finder(n, e)
            for p in range(2):
                index = wide(places[e, pl.ds(n + p, 1), :])
                low_index, mine = index & (LANES - 1), (index >> 7) == group

                def point(r):
                    here = pl.ds(r * SUB, SUB)
                    if found is not None:
                        value = found[r * SUB : (r + 1) * SUB, p * LANES : (p + 1) * LANES]
                        if turn > 0:
                            return value
                        return jnp.where(mine, lookup(values[here, :], low_index), value)
                    return lookup(values[here, :], low_index)

                mass = wide(fields[e, at_new, pl.ds(n + p, 1), :])
                for b in parts:
                    value, least, most = blend(point, n + p, e, b)
                    clipped = jnp.minimum(jnp.maximum(value, least), most)
                    for q, kind in enumerate((clipped, most - clipped, clipped - least)):
                        if by_lookup:
                            kind = jnp.where(mine, kind, 0.0)
                        sums[3 * b + q] = sums[3 * b + q] + mass * kind
                        kept[turn, b, q, n + p, :, cols(e)] = kind
        return tuple(sums)

    def begin_pass(i, carry):
        n = 2 * i
        for e in range(groups):
            found = None if e == groups - 1 else far_found(0, half_rows, n, e)
            for p in range(2):
                low_index = wide(places[e, pl.ds(n + p, 1), :]) & (LANES - 1)

                def point(r):
                    here = pl.ds(r * SUB, SUB)
                    if found is None:
                        return lookup(plain[1, here, :], low_index)
                    return found[r * SUB : (r + 1) * SUB, p * LANES : (p + 1) * LANES]

                begun[n + p, :, cols(e)] = half_sum(point, n + p, e, 0)
        return carry

    def pieces():
        yield pl.ds(SUB, tracers - SUB), pl.ds(0, points)
        for h in range(halves):
            yield pl.ds(0, SUB), pl.ds(h * SUB, SUB)

    def arrived(k, piece):
        landed = halo.at[(k, slice(None), *list(pieces())[piece])] if piece <= halves else halo.at[k]
        pltpu.make_async_copy(landed, landed, halo_recv.at[piece]).wait()

    def select(k, rows):
        index = wide(wanted[pl.ds(k, 1), :]) - jnp.where(k == 0, e_dev - BAND, 0)
        index_low, index_high = index & (LANES - 1), index >> 7
        blocks = [halo.at[k, g].reshape(flat, LANES) for g in range(band_groups)]
        found = []
        for r in rows:
            value = lookup(blocks[0][picked_rows(r), :], index_low)
            for g in range(1, band_groups):
                value = jnp.where(
                    index_high == g, lookup(blocks[g][picked_rows(r), :], index_low), value
                )
            found.append(value)
        return found

    def keep(at, start, rows, dense):
        for r in range(0, len(rows), 2) if dense else ():
            for part, item in enumerate(split(rows[r : r + 2])):
                side[at, pl.ds((start + r) * SUB, 2 * SUB), cols(part)] = item
        for r, item in enumerate(rows):
            plain[at, pl.ds((start + r) * SUB, SUB), :] = item

    def receive_rest(k, at, dense):
        keep(at, mains + 2, rest_rows(select(k, range(mains, mains + line))), dense)

    def receive_half(k, h, ranges):
        arrived(k, 1 + h)
        found = select(k, range(h * SUB, h * SUB + SUB))
        ranges = [
            functools.reduce(combine, found + before)
            for combine, before in zip((jnp.minimum, jnp.maximum), ranges)
        ]
        rows = cubic(found[:line]) + cubic(found[line:])
        keep(1, h * half_rows, rows + (ranges if h else []), True)
        return [[item] for item in ranges]

    for sem, filled in enumerate((fields, places, wanted)):
        pltpu.make_async_copy(filled, filled, load_sem.at[sem]).wait()
    pl.semaphore_wait(barrier, jnp.where(at_hub, n_all - 1, 2))
    for k in (near, far):
        ahead = k == 0
        start = jnp.where(ahead, groups - band_groups, 0)
        for piece, where in enumerate(pieces() if k is near else [(pl.ds(0, tracers), pl.ds(0, points))]):
            pltpu.make_async_remote_copy(
                src_ref=fields.at[(pl.ds(start, band_groups), *where)],
                dst_ref=halo.at[(k, slice(None), *where)],
                send_sem=halo_send,
                recv_sem=halo_recv.at[piece if k is near else 1 + halves],
                device_id=(jnp.where(ahead, right[0], left[0]), me_l),
                device_id_type=MESH,
            ).start()

    @pl.when(at_hub)
    def _():
        def admit(other, carry):
            signal(ready, lax.div(other, n_lev), lax.rem(other, n_lev))
            return carry

        lax.fori_loop(0, n_all - 1, admit, 0)

    prepare()
    zero = jnp.zeros((SUB, LANES), jnp.float32)
    sums = lax.fori_loop(
        0, steps, functools.partial(gather_pass, own_found, spare, groups - 1, 0, (0, 1), interpolate), (zero,) * 6, unroll=UNROLL
    )

    lane = lax.broadcasted_iota(jnp.int32, (SUB, LANES), 1)
    row = lax.broadcasted_iota(jnp.int32, (SUB, LANES), 0)
    old_main = jnp.zeros((SUB, LANES), jnp.float32)
    for g in range(groups):
        block = fields.at[g].reshape((tracers + 4) * points, LANES)
        for j in range(mains):
            old_main += block[picked_rows(j), :] * wide(fields[g, at_old, pl.ds(j, 1), :])
    old_rest = jnp.zeros((SUB, LANES), jnp.float32)
    for t in range(SUB, tracers):
        product = sum(fields[g, t] * fields[g, at_old] for g in range(groups))
        total = jnp.sum(product, axis=0, keepdims=True)
        old_rest = jnp.where(row == line * (t - SUB), wide(total), old_rest)

    arrived(near, 1 + halves)
    receive_rest(near, 0, True)
    keep(0, 0, main_rows(select(near, range(mains))), True)
    sums = lax.fori_loop(
        0,
        steps,
        functools.partial(gather_pass, functools.partial(near_found, near), plain.at[0], groups + near, 1, (0, 1), interpolate),
        sums,
        unroll=UNROLL,
    )
    lax.fori_loop(0, steps, functools.partial(foresee, far), 0, unroll=2)
    arrived(far, 0)
    receive_rest(far, 1, False)
    sums = lax.fori_loop(
        0, steps, functools.partial(gather_pass, None, plain.at[1], groups + far, 2, (1,), interpolate), sums, unroll=UNROLL
    )
    ranges = receive_half(far, 0, [[], []])
    lax.fori_loop(0, steps, begin_pass, 0, unroll=UNROLL)
    receive_half(far, 1, ranges)
    finder = functools.partial(far_found, half_rows, half_rows + 2)
    values = plain.at[1, pl.ds(half_rows * SUB, (half_rows + 2) * SUB), :]
    sums = lax.fori_loop(
        0, steps, functools.partial(gather_pass, finder, values, groups + far, 2, (0,), end_sum), sums, unroll=UNROLL
    )

    half = LANES // 2
    deficit = room = jnp.zeros((SUB, LANES), jnp.float32)
    for b, old in enumerate((old_main, old_rest)):
        gap, up, down = [
            jnp.sum(item, axis=1, keepdims=True) for item in (old - sums[3 * b], sums[3 * b + 1], sums[3 * b + 2])
        ]
        here, there = lane == b * SUB + row, lane == half + b * SUB + row
        deficit = jnp.where(jnp.logical_or(here, there), gap, deficit)
        room = jnp.where(here, up, jnp.where(there, down, room))
    packed = [jnp.sum(item, axis=0, keepdims=True) for item in (deficit, room)]
    for x in range(2):
        message[pl.ds(x, 1), :] = packed[x]

    @pl.when(jnp.logical_not(at_hub))
    def _():
        pl.semaphore_wait(ready, 1)

    def tell(place, carry):
        other = place + jnp.where(place >= me, 1, 0)
        pltpu.make_async_remote_copy(
            src_ref=message,
            dst_ref=heard.at[me - jnp.where(place < me, 1, 0)],
            send_sem=sum_send,
            recv_sem=sum_recv,
            device_id=(lax.div(other, n_lev), lax.rem(other, n_lev)),
            device_id_type=MESH,
        ).start()
        return carry

    lax.fori_loop(0, n_all - 1, tell, 0)

    def arrange(n, carry):
        for e in range(groups):
            for q in range(3):
                main, rest = [
                    sum(kept[turn, b, q, n, :, cols(e)] for turn in range(3)) for b in range(2)
                ]
                stage[q, e, pl.ds(n, SUB, stride=points), :] = main
                for t in range(SUB, tracers):
                    at = line * (t - SUB)
                    stage[q, e, pl.ds(t * points + n, 1), :] = rest[at : at + 1]
        return carry

    lax.fori_loop(0, points, arrange, 0, unroll=2)
    pltpu.make_async_copy(halo, halo, halo_send).wait()
    pltpu.make_async_copy(heard, heard, sum_recv).wait()
    totals = []
    for x in range(2):
        if n_all <= 64:
            terms = [wide(packed[x])] + [wide(heard[k, pl.ds(x, 1), :]) for k in range(n_all - 1)]
            while len(terms) > 1:
                terms = [sum(terms[k : k + 2]) for k in range(0, len(terms), 2)]
            totals.append(terms[0])
        else:
            totals.append(
                lax.fori_loop(
                    0, n_all - 1, lambda k, acc: acc + wide(heard[k, pl.ds(x, 1), :]), wide(packed[x])
                )
            )
    shortfall, room = totals
    raises = (shortfall >= 0) == (lane < half)
    gain = jnp.where(raises, shortfall / room, 0.0)
    for b in range(2):
        for x in range(2):
            column = jnp.where(lane == half * x + b * SUB + row, gain, 0.0)
            gains[b, x] = jnp.broadcast_to(jnp.sum(column, axis=1, keepdims=True), (SUB, LANES))
    for t in range(tracers):
        b, at = (0, t) if t < SUB else (1, line * (t - SUB))
        up, down = [wide(gains[b, x, pl.ds(at, 1), :]) for x in range(2)]
        for g in range(groups):
            for h in range(halves):
                rows = pl.ds(t * points + h * SUB, SUB)
                moved = up * stage[1, g, rows, :] + down * stage[2, g, rows, :]
                out[rows, cols(g)] = stage[0, g, rows, :] + moved
    pltpu.make_async_copy(heard, heard, sum_send).wait()


def solution(mesh):
    sizes = (mesh.shape["sfc"], mesh.shape["lev"])
    n_all = sizes[0] * sizes[1]

    def on_device(tracer_old, air_old, air_new, dep_coord, dep_slot, fetch_list):
        levels, tracers, points, e_dev = tracer_old.shape
        cap = fetch_list.shape[2]
        assert levels == 1 and cap == LANES and tracers == SUB + 2 and points == 16
        assert e_dev // LANES % 2 == 1 and sizes[0] % 2 == 0
        rows = tracers * points
        groups, halves = e_dev // LANES, points // SUB
        tall, line = (points + 8) * SUB, 4
        vmem = pl.BlockSpec(memory_space=pltpu.VMEM)
        result = pl.pallas_call(
            functools.partial(kernel, sizes),
            out_shape=pltpu.VMEM((rows, e_dev), jnp.float32),
            in_specs=[pl.BlockSpec(memory_space=pl.ANY)] * 6,
            out_specs=vmem,
            scratch_shapes=[
                pltpu.VMEM((groups, tracers + 4, points, LANES), jnp.float32),
                pltpu.VMEM((3, groups, rows, LANES), jnp.float32),
                pltpu.VMEM(((groups - 1) * tall, 2 * LANES), jnp.bfloat16),
                pltpu.VMEM((tall, LANES), jnp.float32),
                pltpu.VMEM((2, BAND // LANES, tracers, points, LANES), jnp.float32),
                pltpu.VMEM((2, tall, 2 * LANES), jnp.bfloat16),
                pltpu.VMEM((2, tall, LANES), jnp.float32),
                pltpu.VMEM((points // 2, groups - 1, LANES, 2 * LANES), jnp.bfloat16),
                pltpu.VMEM((groups, points * SUB, LANES), jnp.float32),
                pltpu.VMEM((line, groups, points, LANES), jnp.float32),
                pltpu.VMEM((points, SUB, e_dev), jnp.float32),
                pltpu.VMEM((groups, points, LANES), jnp.int32),
                pltpu.VMEM((2, cap), jnp.int32),
                pltpu.VMEM((3, 2, 3, points, SUB, e_dev), jnp.float32),
                pltpu.VMEM((2, 2, SUB, LANES), jnp.float32),
                pltpu.VMEM((2, LANES), jnp.float32),
                pltpu.VMEM((n_all - 1, 2, LANES), jnp.float32),
                pltpu.SemaphoreType.DMA((3,)),
                pltpu.SemaphoreType.DMA,
                pltpu.SemaphoreType.DMA((2 + halves,)),
                pltpu.SemaphoreType.DMA,
                pltpu.SemaphoreType.DMA,
                pltpu.SemaphoreType.REGULAR,
            ],
            compiler_params=pltpu.CompilerParams(collective_id=0, has_side_effects=True),
            name="transport",
        )(
            tracer_old.reshape(tracers, points, e_dev),
            air_old.reshape(points, e_dev),
            air_new.reshape(points, e_dev),
            dep_coord.reshape(2, points, e_dev),
            dep_slot.reshape(points, e_dev),
            fetch_list.reshape(2, cap),
        )
        return result.reshape(levels, tracers, points, e_dev)

    return jax.shard_map(
        on_device,
        mesh=mesh,
        in_specs=(
            P("lev", None, None, "sfc"),
            P("lev", None, "sfc"),
            P("lev", None, "sfc"),
            P(None, "lev", None, "sfc"),
            P("lev", None, "sfc"),
            P("sfc", None, None),
        ),
        out_specs=P("lev", None, None, "sfc"),
        check_vma=False,
    )
```

```python
import functools
import math

import jax
import jax.numpy as jnp
from jax import lax
from jax.experimental import pallas as pl
from jax.experimental.pallas import tpu as pltpu
from jax.sharding import PartitionSpec as P

BAND = 256
LANES = 128
SUB = 8
NODES = (-1.0, -0.4472135954999579, 0.4472135954999579, 1.0)
UNROLL = 8
MESH = pl.DeviceIdType.MESH


def basis(coord):
    terms = []
    for first in range(4):
        term = None
        scale = 1.0
        for other in range(4):
            if other != first:
                factor = coord - NODES[other]
                term = factor if term is None else term * factor
                scale = scale / (NODES[first] - NODES[other])
        terms.append(term * scale)
    return terms


def cubic(values):
    outer, inner = values[3] + values[0], values[2] + values[1]
    wide_odd, near_odd = values[3] - values[0], (values[2] - values[1]) * math.sqrt(5.0)
    return [
        0.625 * inner - 0.125 * outer,
        0.625 * near_odd - 0.125 * wide_odd,
        0.625 * (outer - inner),
        0.625 * (wide_odd - near_odd),
    ]


def horner(terms, at):
    total = terms[3]
    for term in terms[2::-1]:
        total = total * at + term
    return total


def lookup(values, index):
    return jnp.take_along_axis(values, index, axis=1, mode="promise_in_bounds")


def wide(row):
    return jnp.broadcast_to(row, (SUB, LANES))


def split(pair):
    value = jnp.concatenate(pair, axis=0)
    high = value.astype(jnp.bfloat16)
    return high, (value - high.astype(jnp.float32)).astype(jnp.bfloat16)


def folded(values, combine):
    for shift in (1, 2):
        values = combine(values, pltpu.roll(values, SUB - shift, 0))
    return values


def kernel(
    sizes, tr, air_old, air_new, coord, slot, fetch, out,
    fields, stage, table, spare, halo, side, plain, picks, along, lagrange, begun, places, wanted,
    kept, gains, message, heard, load_sem, halo_send, halo_recv, sum_send, sum_recv, ready,
):
    n_sfc, n_lev = sizes
    n_all = n_sfc * n_lev
    points = slot.shape[0]
    tracers, _, e_dev = tr.shape
    groups = e_dev // LANES
    halves = points // SUB
    mains = points
    line = 4
    flat = tracers * points
    kinds = mains + line + 4
    tall = kinds * SUB
    half_rows = mains // 2
    band_groups = BAND // LANES
    steps = points // 2
    me_s, me_l = lax.axis_index("sfc"), lax.axis_index("lev")
    me = me_s * n_lev + me_l
    right = (jnp.where(me_s == n_sfc - 1, 0, me_s + 1), me_l)
    left = (jnp.where(me_s == 0, n_sfc - 1, me_s - 1), me_l)
    hub_s, hub_l = n_sfc - 1, n_lev - 1
    at_hub = me == n_all - 1
    far = lax.rem(me_s, 2)
    near = 1 - far
    barrier = pltpu.get_barrier_semaphore()

    def signal(sem, s, l):
        pl.semaphore_signal(sem, inc=1, device_id=(s, l), device_id_type=MESH)

    for other_s, other_l in (right, left):

        @pl.when(jnp.logical_or(other_s != hub_s, other_l != hub_l))
        def _():
            signal(barrier, other_s, other_l)

    @pl.when(jnp.logical_not(at_hub))
    def _():
        signal(barrier, hub_s, hub_l)

    def cols(group):
        return pl.ds(group * LANES, LANES)

    def load(source, target, sem):
        pltpu.make_async_copy(source, target, load_sem.at[sem]).start()

    at_coord, at_new, at_old = tracers, tracers + 2, tracers + 3
    for g in range(groups):
        load(tr.at[:, :, cols(g)], fields.at[g, pl.ds(0, tracers)], 0)
    for g in range(groups):
        load(slot.at[:, cols(g)], places.at[g], 1)
        load(coord.at[:, :, cols(g)], fields.at[g, pl.ds(at_coord, 2)], 0)
    for g in range(groups):
        load(air_old.at[:, cols(g)], fields.at[g, at_old], 0)
        load(air_new.at[:, cols(g)], fields.at[g, at_new], 0)
    load(fetch, wanted, 2)

    def picked_rows(r):
        if r < mains:
            return pl.ds(r, SUB, stride=points)
        return pl.ds(SUB * points + (r - mains), SUB, stride=line)

    def main_rows(main):
        along_b = [cubic(main[line * i : line * i + line]) for i in range(line)]
        along_a = [cubic([along_b[i][m] for i in range(line)]) for m in range(line)]
        ranges = [functools.reduce(combine, main) for combine in (jnp.minimum, jnp.maximum)]
        return [along_a[m][i] for i in range(line) for m in range(line)] + ranges

    def rest_rows(rest):
        return cubic(rest) + [
            folded(functools.reduce(combine, rest), combine) for combine in (jnp.minimum, jnp.maximum)
        ]

    def prepare():
        for g in range(groups):
            block = fields.at[g].reshape((tracers + 4) * points, LANES)
            found = [block[picked_rows(r), :] for r in range(mains + line)]
            rows = main_rows(found[:mains]) + rest_rows(found[mains:])
            if g == groups - 1:
                for r, item in enumerate(rows):
                    spare[pl.ds(r * SUB, SUB), :] = item
                continue
            for r in range(0, kinds, 2):
                for part, item in enumerate(split(rows[r : r + 2])):
                    at = pl.ds((g // 2 * 2 + part) * tall + r * SUB, 2 * SUB)
                    table[at, cols(g % 2)] = item
        for g in range(groups):
            for i, term in enumerate(basis(fields[g, at_coord])):
                lagrange[i, g] = term
                for s in (i, i + line):
                    along[g, pl.ds(s, points, stride=SUB), :] = term

    def interpolate(point, n, e, b):
        at_a, at_b = [wide(fields[e, at_coord + x, pl.ds(n, 1), :]) for x in range(2)]
        if b == 0:
            inner = [horner([point(line * i + m) for m in range(line)], at_b) for i in range(line)]
            return horner(inner, at_a), point(mains), point(mains + 1)
        rest = horner([point(mains + 2 + m) for m in range(line)], at_b)
        rest = folded(rest * along[e, pl.ds(n * SUB, SUB), :], jnp.add)
        return rest, point(mains + 2 + line), point(mains + 3 + line)

    def half_sum(point, n, e, h):
        at_b = wide(fields[e, at_coord + 1, pl.ds(n, 1), :])
        pair = [
            horner([point(line * x + m) for m in range(line)], at_b)
            * wide(lagrange[2 * h + x, e, pl.ds(n, 1), :])
            for x in range(2)
        ]
        return pair[0] + pair[1]

    def end_sum(point, n, e, b):
        value = begun[n, :, cols(e)] + half_sum(point, n, e, 1)
        return value, point(half_rows), point(half_rows + 1)

    number = lax.broadcasted_iota(jnp.int32, (LANES, LANES), 0).astype(jnp.float32).astype(jnp.bfloat16)

    def chosen(n, e, group):
        columns = []
        for p in range(2):
            row = wide(places[e, pl.ds(n + p, 1), :])
            spot = jnp.where(row >> 7 == group, row & (LANES - 1), -1).astype(jnp.float32)
            spot = jnp.concatenate([spot, spot], axis=0).astype(jnp.bfloat16)
            match = number == jnp.concatenate([spot] * SUB, axis=0)
            columns.append(jnp.where(match, jnp.bfloat16(1), jnp.bfloat16(0)))
        return jnp.concatenate(columns, axis=1)

    def times(values, pick):
        return jnp.dot(values, pick, preferred_element_type=jnp.float32)

    def own_found(n, e):
        total = None
        for g in range(0, groups - 1, 2):
            pick = jnp.concatenate([chosen(n, e, g + x) for x in range(2)], axis=0)
            both = times(table[pl.ds(g * tall, 2 * tall), :], pick)
            found = both[:tall] + both[tall:]
            total = found if total is None else total + found
        return total

    def near_found(k, n, e):
        one = chosen(n, e, groups + k)
        return times(side[0], jnp.concatenate([one, one], axis=0))

    def far_found(first, count, n, e):
        one = picks[n // 2, e]
        values = side[1, pl.ds(first * SUB, count * SUB), :]
        return times(values, jnp.concatenate([one, one], axis=0))

    def foresee(k, i, carry):
        for e in range(groups - 1):
            picks[i, e] = chosen(2 * i, e, groups + k)
        return carry

    def gather_pass(finder, values, group, turn, parts, blend, i, carry):
        sums = list(carry)
        n = 2 * i
        for e in range(groups):
            by_lookup = finder is None or (turn > 0 and e == groups - 1)
            found = None if by_lookup else finder(n, e)
            for p in range(2):
                index = wide(places[e, pl.ds(n + p, 1), :])
                low_index, mine = index & (LANES - 1), (index >> 7) == group

                def point(r):
                    here = pl.ds(r * SUB, SUB)
                    if found is not None:
                        value = found[r * SUB : (r + 1) * SUB, p * LANES : (p + 1) * LANES]
                        if turn > 0:
                            return value
                        return jnp.where(mine, lookup(values[here, :], low_index), value)
                    return lookup(values[here, :], low_index)

                mass = wide(fields[e, at_new, pl.ds(n + p, 1), :])
                for b in parts:
                    value, least, most = blend(point, n + p, e, b)
                    clipped = jnp.minimum(jnp.maximum(value, least), most)
                    for q, kind in enumerate((clipped, most - clipped, clipped - least)):
                        if by_lookup:
                            kind = jnp.where(mine, kind, 0.0)
                        sums[3 * b + q] = sums[3 * b + q] + mass * kind
                        kept[turn, b, q, n + p, :, cols(e)] = kind
        return tuple(sums)

    def begin_pass(i, carry):
        n = 2 * i
        for e in range(groups):
            found = None if e == groups - 1 else far_found(0, half_rows, n, e)
            for p in range(2):
                low_index = wide(places[e, pl.ds(n + p, 1), :]) & (LANES - 1)

                def point(r):
                    here = pl.ds(r * SUB, SUB)
                    if found is None:
                        return lookup(plain[1, here, :], low_index)
                    return found[r * SUB : (r + 1) * SUB, p * LANES : (p + 1) * LANES]

                begun[n + p, :, cols(e)] = half_sum(point, n + p, e, 0)
        return carry

    def pieces():
        yield pl.ds(SUB, tracers - SUB), pl.ds(0, points)
        for h in range(halves):
            yield pl.ds(0, SUB), pl.ds(h * SUB, SUB)

    def arrived(k, piece):
        landed = halo.at[(k, slice(None), *list(pieces())[piece])] if piece <= halves else halo.at[k]
        pltpu.make_async_copy(landed, landed, halo_recv.at[piece]).wait()

    def select(k, rows):
        index = wide(wanted[pl.ds(k, 1), :]) - jnp.where(k == 0, e_dev - BAND, 0)
        index_low, index_high = index & (LANES - 1), index >> 7
        blocks = [halo.at[k, g].reshape(flat, LANES) for g in range(band_groups)]
        found = []
        for r in rows:
            value = lookup(blocks[0][picked_rows(r), :], index_low)
            for g in range(1, band_groups):
                value = jnp.where(
                    index_high == g, lookup(blocks[g][picked_rows(r), :], index_low), value
                )
            found.append(value)
        return found

    def keep(at, start, rows, dense):
        for r in range(0, len(rows), 2) if dense else ():
            for part, item in enumerate(split(rows[r : r + 2])):
                side[at, pl.ds((start + r) * SUB, 2 * SUB), cols(part)] = item
        for r, item in enumerate(rows):
            plain[at, pl.ds((start + r) * SUB, SUB), :] = item

    def receive_rest(k, at, dense):
        keep(at, mains + 2, rest_rows(select(k, range(mains, mains + line))), dense)

    def receive_half(k, h, ranges):
        arrived(k, 1 + h)
        found = select(k, range(h * SUB, h * SUB + SUB))
        ranges = [
            functools.reduce(combine, found + before)
            for combine, before in zip((jnp.minimum, jnp.maximum), ranges)
        ]
        rows = cubic(found[:line]) + cubic(found[line:])
        keep(1, h * half_rows, rows + (ranges if h else []), True)
        return [[item] for item in ranges]

    for sem, filled in enumerate((fields, places, wanted)):
        pltpu.make_async_copy(filled, filled, load_sem.at[sem]).wait()
    pl.semaphore_wait(barrier, jnp.where(at_hub, n_all - 1, 2))
    for k in (near, far):
        ahead = k == 0
        start = jnp.where(ahead, groups - band_groups, 0)
        for piece, where in enumerate(pieces() if k is near else [(pl.ds(0, tracers), pl.ds(0, points))]):
            pltpu.make_async_remote_copy(
                src_ref=fields.at[(pl.ds(start, band_groups), *where)],
                dst_ref=halo.at[(k, slice(None), *where)],
                send_sem=halo_send,
                recv_sem=halo_recv.at[piece if k is near else 1 + halves],
                device_id=(jnp.where(ahead, right[0], left[0]), me_l),
                device_id_type=MESH,
            ).start()

    @pl.when(at_hub)
    def _():
        def admit(other, carry):
            signal(ready, lax.div(other, n_lev), lax.rem(other, n_lev))
            return carry

        lax.fori_loop(0, n_all - 1, admit, 0)

    prepare()
    zero = jnp.zeros((SUB, LANES), jnp.float32)
    sums = lax.fori_loop(
        0, steps, functools.partial(gather_pass, own_found, spare, groups - 1, 0, (0, 1), interpolate), (zero,) * 6, unroll=UNROLL
    )

    lane = lax.broadcasted_iota(jnp.int32, (SUB, LANES), 1)
    row = lax.broadcasted_iota(jnp.int32, (SUB, LANES), 0)
    old_main = jnp.zeros((SUB, LANES), jnp.float32)
    for g in range(groups):
        block = fields.at[g].reshape((tracers + 4) * points, LANES)
        for j in range(mains):
            old_main += block[picked_rows(j), :] * wide(fields[g, at_old, pl.ds(j, 1), :])
    old_rest = jnp.zeros((SUB, LANES), jnp.float32)
    for t in range(SUB, tracers):
        product = sum(fields[g, t] * fields[g, at_old] for g in range(groups))
        total = jnp.sum(product, axis=0, keepdims=True)
        old_rest = jnp.where(row == line * (t - SUB), wide(total), old_rest)

    arrived(near, 1 + halves)
    receive_rest(near, 0, True)
    keep(0, 0, main_rows(select(near, range(mains))), True)
    sums = lax.fori_loop(
        0,
        steps,
        functools.partial(gather_pass, functools.partial(near_found, near), plain.at[0], groups + near, 1, (0, 1), interpolate),
        sums,
        unroll=UNROLL,
    )
    lax.fori_loop(0, steps, functools.partial(foresee, far), 0, unroll=2)
    arrived(far, 0)
    receive_rest(far, 1, False)
    sums = lax.fori_loop(
        0, steps, functools.partial(gather_pass, None, plain.at[1], groups + far, 2, (1,), interpolate), sums, unroll=UNROLL
    )
    half = LANES // 2

    def add_masses(b, old, sums, deficit, room):
        gap, up, down = [
            jnp.sum(item, axis=1, keepdims=True) for item in (old - sums[3 * b], sums[3 * b + 1], sums[3 * b + 2])
        ]
        here, there = lane == b * SUB + row, lane == half + b * SUB + row
        deficit = jnp.where(jnp.logical_or(here, there), gap, deficit)
        return deficit, jnp.where(here, up, jnp.where(there, down, room))

    ranges = receive_half(far, 0, [[], []])
    deficit, room = add_masses(1, old_rest, sums, zero, zero)
    lax.fori_loop(0, steps, begin_pass, 0, unroll=UNROLL)
    receive_half(far, 1, ranges)
    finder = functools.partial(far_found, half_rows, half_rows + 2)
    values = plain.at[1, pl.ds(half_rows * SUB, (half_rows + 2) * SUB), :]
    sums = lax.fori_loop(
        0, steps, functools.partial(gather_pass, finder, values, groups + far, 2, (0,), end_sum), sums, unroll=UNROLL
    )

    deficit, room = add_masses(0, old_main, sums, deficit, room)
    packed = [jnp.sum(item, axis=0, keepdims=True) for item in (deficit, room)]
    for x in range(2):
        message[pl.ds(x, 1), :] = packed[x]

    @pl.when(jnp.logical_not(at_hub))
    def _():
        pl.semaphore_wait(ready, 1)

    def tell(place, carry):
        other = place + jnp.where(place >= me, 1, 0)
        pltpu.make_async_remote_copy(
            src_ref=message,
            dst_ref=heard.at[me - jnp.where(place < me, 1, 0)],
            send_sem=sum_send,
            recv_sem=sum_recv,
            device_id=(lax.div(other, n_lev), lax.rem(other, n_lev)),
            device_id_type=MESH,
        ).start()
        return carry

    lax.fori_loop(0, n_all - 1, tell, 0)

    def arrange(n, carry):
        for e in range(groups):
            for q in range(3):
                main, rest = [
                    sum(kept[turn, b, q, n, :, cols(e)] for turn in range(3)) for b in range(2)
                ]
                stage[q, e, pl.ds(n, SUB, stride=points), :] = main
                for t in range(SUB, tracers):
                    at = line * (t - SUB)
                    stage[q, e, pl.ds(t * points + n, 1), :] = rest[at : at + 1]
        return carry

    lax.fori_loop(0, points, arrange, 0, unroll=2)
    pltpu.make_async_copy(halo, halo, halo_send).wait()
    pltpu.make_async_copy(heard, heard, sum_recv).wait()
    totals = []
    for x in range(2):
        if n_all <= 64:
            terms = [wide(packed[x])] + [wide(heard[k, pl.ds(x, 1), :]) for k in range(n_all - 1)]
            while len(terms) > 1:
                terms = [sum(terms[k : k + 2]) for k in range(0, len(terms), 2)]
            totals.append(terms[0])
        else:
            totals.append(
                lax.fori_loop(
                    0, n_all - 1, lambda k, acc: acc + wide(heard[k, pl.ds(x, 1), :]), wide(packed[x])
                )
            )
    shortfall, room = totals
    raises = (shortfall >= 0) == (lane < half)
    gain = jnp.where(raises, shortfall / room, 0.0)
    for b in range(2):
        for x in range(2):
            column = jnp.where(lane == half * x + b * SUB + row, gain, 0.0)
            gains[b, x] = jnp.broadcast_to(jnp.sum(column, axis=1, keepdims=True), (SUB, LANES))
    for t in range(tracers):
        b, at = (0, t) if t < SUB else (1, line * (t - SUB))
        up, down = [wide(gains[b, x, pl.ds(at, 1), :]) for x in range(2)]
        for g in range(groups):
            for h in range(halves):
                rows = pl.ds(t * points + h * SUB, SUB)
                moved = up * stage[1, g, rows, :] + down * stage[2, g, rows, :]
                out[rows, cols(g)] = stage[0, g, rows, :] + moved
    pltpu.make_async_copy(heard, heard, sum_send).wait()


def solution(mesh):
    sizes = (mesh.shape["sfc"], mesh.shape["lev"])
    n_all = sizes[0] * sizes[1]

    def on_device(tracer_old, air_old, air_new, dep_coord, dep_slot, fetch_list):
        levels, tracers, points, e_dev = tracer_old.shape
        cap = fetch_list.shape[2]
        assert levels == 1 and cap == LANES and tracers == SUB + 2 and points == 16
        assert e_dev // LANES % 2 == 1 and sizes[0] % 2 == 0
        rows = tracers * points
        groups, halves = e_dev // LANES, points // SUB
        tall, line = (points + 8) * SUB, 4
        vmem = pl.BlockSpec(memory_space=pltpu.VMEM)
        result = pl.pallas_call(
            functools.partial(kernel, sizes),
            out_shape=pltpu.VMEM((rows, e_dev), jnp.float32),
            in_specs=[pl.BlockSpec(memory_space=pl.ANY)] * 6,
            out_specs=vmem,
            scratch_shapes=[
                pltpu.VMEM((groups, tracers + 4, points, LANES), jnp.float32),
                pltpu.VMEM((3, groups, rows, LANES), jnp.float32),
                pltpu.VMEM(((groups - 1) * tall, 2 * LANES), jnp.bfloat16),
                pltpu.VMEM((tall, LANES), jnp.float32),
                pltpu.VMEM((2, BAND // LANES, tracers, points, LANES), jnp.float32),
                pltpu.VMEM((2, tall, 2 * LANES), jnp.bfloat16),
                pltpu.VMEM((2, tall, LANES), jnp.float32),
                pltpu.VMEM((points // 2, groups - 1, LANES, 2 * LANES), jnp.bfloat16),
                pltpu.VMEM((groups, points * SUB, LANES), jnp.float32),
                pltpu.VMEM((line, groups, points, LANES), jnp.float32),
                pltpu.VMEM((points, SUB, e_dev), jnp.float32),
                pltpu.VMEM((groups, points, LANES), jnp.int32),
                pltpu.VMEM((2, cap), jnp.int32),
                pltpu.VMEM((3, 2, 3, points, SUB, e_dev), jnp.float32),
                pltpu.VMEM((2, 2, SUB, LANES), jnp.float32),
                pltpu.VMEM((2, LANES), jnp.float32),
                pltpu.VMEM((n_all - 1, 2, LANES), jnp.float32),
                pltpu.SemaphoreType.DMA((3,)),
                pltpu.SemaphoreType.DMA,
                pltpu.SemaphoreType.DMA((2 + halves,)),
                pltpu.SemaphoreType.DMA,
                pltpu.SemaphoreType.DMA,
                pltpu.SemaphoreType.REGULAR,
            ],
            compiler_params=pltpu.CompilerParams(collective_id=0, has_side_effects=True),
            name="transport",
        )(
            tracer_old.reshape(tracers, points, e_dev),
            air_old.reshape(points, e_dev),
            air_new.reshape(points, e_dev),
            dep_coord.reshape(2, points, e_dev),
            dep_slot.reshape(points, e_dev),
            fetch_list.reshape(2, cap),
        )
        return result.reshape(levels, tracers, points, e_dev)

    return jax.shard_map(
        on_device,
        mesh=mesh,
        in_specs=(
            P("lev", None, None, "sfc"),
            P("lev", None, "sfc"),
            P("lev", None, "sfc"),
            P(None, "lev", None, "sfc"),
            P("lev", None, "sfc"),
            P("sfc", None, None),
        ),
        out_specs=P("lev", None, None, "sfc"),
        check_vma=False,
    )
```
